256 devices in a mesh: ctx: 32 (over z, y), help: 8 (over x, core).
Axes of the slice: x: 4, y: 4, z: 8, core: 2. Of those that a mesh axis runs over, the one named last changes fastest.
Arguments:
- query_rows: bfloat16 [1, 32768, 2048], P(None, ('ctx', 'help')), may hold values from -126 to 126
- key_rows: bfloat16 [1, 32768, 2048], P(None, 'ctx'), may hold values from -6.5 to 6.5
- value_rows: bfloat16 [1, 32768, 2048], P(None, 'ctx'), may hold values from -6 to 6
- output_grad: bfloat16 [1, 32768, 2048], P(None, ('ctx', 'help')), may hold values from -96 to 96
- block_choice: int32 [1, 32768, 2], P(None, ('ctx', 'help')), may hold values from 0 to 31, as said below
Outputs:
- query_grad: bfloat16 [1, 32768, 2048], P(None, ('ctx', 'help'))
- key_grad: bfloat16 [1, 32768, 2048], P(None, ('ctx', 'help'))
- value_grad: bfloat16 [1, 32768, 2048], P(None, ('ctx', 'help'))
The draws below stay inside these ranges and needn't reach their ends.
Inputs may be any that keep to these rules, and one draw needn't show every extreme that they name: `block_choice`: an entry names a block only where it is below the token's own block index; the entries of a token that name blocks name different blocks. In each aligned run of 128 rows of one sequence (the rows of one device) no block is named more than 8 times, and the devices of a sequence's third block name each of its first two blocks exactly 8 times. Blocks early in a sequence are named by the tokens of more blocks than late ones.
All inputs are finite; a program needn't handle non-finite values.
Results may differ from the reference program's by a relative error of at most 0.01.
Values may be sent and summed in bfloat16 or wider, within the bound.
No kernel may reach another device: no remote copies, remote signals or barrier semaphores. Data moves between devices by JAX's collectives and lax.ppermute only.
A program may use at most 192 MiB of HBM per device.

```python
import jax
import jax.numpy as jnp
from jax import lax

HEADS = 16
HEAD_DIM = 128
BLOCK = 1024
ROUTED = 2
SEQUENCES = 1
WIDTH = 2048
BLOCKS = 32
SEQ_LEN = 32768
ROWS_DEV = 128
MOST = 8
N_CTX = 32
N_HELP = 8


def base_keys(key):
    drawn = jax.random.normal(jax.random.fold_in(key, 71), (SEQUENCES, SEQ_LEN, WIDTH), jnp.float32)
    return jnp.clip(drawn, -6.0, 6.0)


def draw_key_rows(key, part):
    keys_base = base_keys(key)
    return keys_base.astype(jnp.bfloat16)


def draw_query_rows(key, part):
    values = jnp.clip(jax.random.normal(jax.random.fold_in(key, 73), (SEQUENCES, SEQ_LEN, WIDTH), jnp.float32), -6.0, 6.0)
    return values.astype(jnp.bfloat16)


def draw_block_choice(key, part):
    group_count = SEQ_LEN // ROWS_DEV
    per_route = MOST // 2
    layout = (SEQUENCES, group_count, ROWS_DEV)
    narrow = (SEQUENCES, group_count, 1)
    scores = jax.random.randint(jax.random.fold_in(key, 81), layout, 0, 1 << 20) * ROWS_DEV + jnp.arange(ROWS_DEV, dtype=jnp.int32)
    sort_order = jnp.argsort(scores, axis=2, stable=True)
    rank_of = jnp.argsort(sort_order, axis=2, stable=True).astype(jnp.int32)
    own_block = (jnp.arange(group_count, dtype=jnp.int32) * ROWS_DEV // BLOCK)[None, :, None]
    modulus = jnp.maximum(own_block, 1)
    start_one = jax.random.randint(jax.random.fold_in(key, 82), narrow, 0, 1 << 20) % modulus
    start_two = start_one + 1 + jax.random.randint(jax.random.fold_in(key, 83), narrow, 0, 1 << 20) % jnp.maximum(own_block - 1, 1)
    ceiling = own_block * per_route
    floor_part = ceiling // 2

    def limit_of(salt_value):
        drawn_limit = floor_part + jax.random.randint(jax.random.fold_in(key, salt_value), narrow, 0, 1 << 20) % (ceiling - floor_part + 1)
        return jnp.where(own_block == 2, ceiling, drawn_limit)
    route_one = jnp.where((rank_of < limit_of(84)) & (own_block >= 1), (start_one + rank_of) % modulus, BLOCKS - 1)
    route_two = jnp.where((rank_of < limit_of(85)) & (own_block >= 2), (start_two + rank_of) % modulus, BLOCKS - 1)
    return jnp.stack([route_one, route_two], axis=3).reshape(SEQUENCES, SEQ_LEN, ROUTED).astype(jnp.int32)


def block_levels(stream_key, shape, split, least, largest):
    factor_of = 1.0
    for dim, parts in split:
        steps = jax.random.uniform(jax.random.fold_in(jax.random.fold_in(stream_key, 6), dim), (parts,), jnp.float32, least / len(split), largest / len(split))
        factor_of = factor_of * jnp.repeat(jnp.exp(steps), shape[dim] // parts).reshape((-1,) + (1,) * (len(shape) - 1 - dim))
    return factor_of


def normal_values(stream_key, extent, spread, bound, split=(), kind=jnp.bfloat16):
    gain = block_levels(stream_key, extent, split, -0.22, 0.18) if split else 1.0
    values = jax.random.normal(stream_key, extent, jnp.float32) * spread * gain
    return jnp.minimum(jnp.maximum(values, -bound), bound).astype(kind)


def setup_inputs(seed: int = 0) -> dict:
    streams_of = jax.random.split(jax.random.key(seed), 6)
    query_rows = draw_query_rows(jax.random.fold_in(streams_of[5], 71), 0)
    key_rows = draw_key_rows(jax.random.fold_in(streams_of[5], 71), 0)
    value_rows = normal_values(streams_of[2], (SEQUENCES, SEQ_LEN, WIDTH), 1.0, 6.0, ((1, 32),))
    output_grad = normal_values(streams_of[3], (SEQUENCES, SEQ_LEN, WIDTH), 16.0, 96.0, ((1, 256),))
    block_choice = draw_block_choice(jax.random.fold_in(streams_of[5], 71), 0)
    return {"query_rows": query_rows, "key_rows": key_rows, "value_rows": value_rows, "output_grad": output_grad, "block_choice": block_choice}


NEGATIVE = -1.0e30


def split_heads(matrix):
    return jnp.transpose(matrix.astype(jnp.float32).reshape(matrix.shape[0], HEADS, HEAD_DIM), (1, 0, 2))


def cell_rows(targets, block_id, helper_id):
    positions = jnp.arange(SEQ_LEN, dtype=jnp.int32)
    groups = (positions % BLOCK) // ROWS_DEV
    chosen = jnp.any(targets == block_id, axis=1) & (groups == helper_id)
    routed = jnp.nonzero(chosen, size=N_CTX * MOST, fill_value=SEQ_LEN)[0].astype(jnp.int32)
    own_offsets = jnp.arange(ROWS_DEV, dtype=jnp.int32) + helper_id * ROWS_DEV
    row_ids = jnp.concatenate([block_id * BLOCK + own_offsets, routed])
    limits = jnp.concatenate([own_offsets, jnp.full((N_CTX * MOST,), BLOCK - 1, jnp.int32)])
    return row_ids, limits


def gather_rows(matrix, row_ids):
    present = row_ids < SEQ_LEN
    picked = matrix[jnp.minimum(row_ids, SEQ_LEN - 1)]
    return jnp.where(present[:, None], picked, jnp.zeros_like(picked))


def cell_statistics(query_block, grad_block, key_block, value_block, limits):
    scaling = HEAD_DIM ** -0.5
    allowed = jnp.arange(BLOCK, dtype=jnp.int32)[None, :] <= limits[:, None]
    scores = jnp.einsum("hrd,hkd->hrk", split_heads(query_block), split_heads(key_block)) * scaling
    scores = jnp.where(allowed, scores, NEGATIVE)
    highest = jnp.max(scores, axis=2)
    weights = jnp.where(allowed, jnp.exp(scores - highest[:, :, None]), 0.0)
    products = jnp.einsum("hrd,hkd->hrk", split_heads(grad_block), split_heads(value_block))
    return highest.T, jnp.sum(weights, axis=2).T, jnp.sum(weights * products, axis=2).T


def cell_gradients(query_block, grad_block, key_block, value_block, limits, log_rows, shifts):
    scaling = HEAD_DIM ** -0.5
    allowed = jnp.arange(BLOCK, dtype=jnp.int32)[None, :] <= limits[:, None]
    queries = split_heads(query_block)
    key_heads = split_heads(key_block)
    grads_out = split_heads(grad_block)
    value_heads = split_heads(value_block)
    scores = jnp.einsum("hrd,hkd->hrk", queries, key_heads) * scaling
    probabilities = jnp.where(allowed, jnp.exp(scores - log_rows.T[:, :, None]), 0.0)
    products = jnp.einsum("hrd,hkd->hrk", grads_out, value_heads)
    mixed = probabilities * (products - shifts.T[:, :, None])
    prob_low = lax.optimization_barrier(probabilities.astype(jnp.bfloat16)).astype(jnp.float32)
    mixed_low = lax.optimization_barrier(mixed.astype(jnp.bfloat16)).astype(jnp.float32)
    value_term = jnp.einsum("hrk,hrd->khd", prob_low, grads_out).reshape(BLOCK, WIDTH)
    key_term = jnp.einsum("hrk,hrd->khd", mixed_low, queries).reshape(BLOCK, WIDTH) * scaling
    query_term = jnp.einsum("hrk,hkd->rhd", mixed_low, key_heads).reshape(query_block.shape[0], WIDTH) * scaling
    return query_term, key_term, value_term


def one_sequence(arrays):
    query_rows, key_rows, value_rows, output_grad, block_choice = arrays
    positions = jnp.arange(SEQ_LEN, dtype=jnp.int32)
    own_blocks = (positions // BLOCK)[:, None]
    targets = jnp.where(block_choice < own_blocks, own_blocks - 1 - block_choice, -1).astype(jnp.int32)

    def collect(running, cell_id):
        block_id = cell_id // N_HELP
        helper_id = cell_id % N_HELP
        row_ids, limits = cell_rows(targets, block_id, helper_id)
        key_block = lax.dynamic_slice_in_dim(key_rows, block_id * BLOCK, BLOCK, 0)
        value_block = lax.dynamic_slice_in_dim(value_rows, block_id * BLOCK, BLOCK, 0)
        new_max, new_norm, new_dot = cell_statistics(gather_rows(query_rows, row_ids), gather_rows(output_grad, row_ids), key_block, value_block, limits)
        safe_ids = jnp.minimum(row_ids, SEQ_LEN - 1)
        old_max = running[0][safe_ids]
        old_norm = running[1][safe_ids]
        old_dot = running[2][safe_ids]
        top_value = jnp.maximum(old_max, new_max)
        old_scale = jnp.exp(old_max - top_value)
        new_scale = jnp.exp(new_max - top_value)
        merged = (top_value, old_norm * old_scale + new_norm * new_scale, old_dot * old_scale + new_dot * new_scale)
        updated = tuple(stored.at[row_ids].set(update, mode="drop") for stored, update in zip(running, merged))
        return updated, None

    initial = (jnp.full((SEQ_LEN, HEADS), NEGATIVE, jnp.float32), jnp.zeros((SEQ_LEN, HEADS), jnp.float32), jnp.zeros((SEQ_LEN, HEADS), jnp.float32))
    gathered = lax.scan(collect, initial, jnp.arange(N_CTX * N_HELP, dtype=jnp.int32))[0]
    log_total = gathered[0] + jnp.log(gathered[1])
    centering = gathered[2] / gathered[1]

    def block_pass(query_acc, block_id):
        key_block = lax.dynamic_slice_in_dim(key_rows, block_id * BLOCK, BLOCK, 0)
        value_block = lax.dynamic_slice_in_dim(value_rows, block_id * BLOCK, BLOCK, 0)

        def helper_pass(running, helper_id):
            query_sum, key_acc, value_acc = running
            row_ids, limits = cell_rows(targets, block_id, helper_id)
            present = (row_ids < SEQ_LEN)[:, None]
            safe_ids = jnp.minimum(row_ids, SEQ_LEN - 1)
            log_rows = jnp.where(present, log_total[safe_ids], 0.0)
            shifts = jnp.where(present, centering[safe_ids], 0.0)
            query_term, key_term, value_term = cell_gradients(gather_rows(query_rows, row_ids), gather_rows(output_grad, row_ids), key_block, value_block, limits, log_rows, shifts)
            key_acc = key_acc + lax.optimization_barrier(key_term.astype(jnp.bfloat16)).astype(jnp.float32)
            value_acc = value_acc + lax.optimization_barrier(value_term.astype(jnp.bfloat16)).astype(jnp.float32)
            query_sum = query_sum.at[row_ids].add(query_term, mode="drop")
            return (query_sum, key_acc, value_acc), None

        zeroed = jnp.zeros((BLOCK, WIDTH), jnp.float32)
        result = lax.scan(helper_pass, (query_acc, zeroed, zeroed), jnp.arange(N_HELP, dtype=jnp.int32))[0]
        return result[0], (result[1].astype(jnp.bfloat16), result[2].astype(jnp.bfloat16))

    query_final, block_grads = lax.scan(block_pass, jnp.zeros((SEQ_LEN, WIDTH), jnp.float32), jnp.arange(BLOCKS, dtype=jnp.int32))
    return query_final.astype(jnp.bfloat16), block_grads[0].reshape(SEQ_LEN, WIDTH), block_grads[1].reshape(SEQ_LEN, WIDTH)


def reference(query_rows, key_rows, value_rows, output_grad, block_choice):
    outputs = lax.map(one_sequence, (query_rows, key_rows, value_rows, output_grad, block_choice))
    return (outputs[0], outputs[1], outputs[2])
```

```python
import functools

import jax
import jax.numpy as jnp
from jax import lax
from jax.experimental import pallas as pl
from jax.experimental.pallas import tpu as pltpu
from jax.sharding import PartitionSpec as P

HEAD_DIM = 128
CAPACITY = 8
NEGATIVE = -1e30
LOG2E = 1.4426950408889634
LN2 = 0.6931471805599453
SCALING = HEAD_DIM ** (-0.5)
INFO = 16
TILE = 256
F32 = jnp.float32
BF16 = jnp.bfloat16


def iota(shape, dim):
    return lax.broadcasted_iota(jnp.int32, shape, dim)


def dot(a, b, ca, cb, precision=None):
    return lax.dot_general(
        a, b, (((ca,), (cb,)), ((), ())), precision=precision, preferred_element_type=F32
    )


def params(**kw):
    return pltpu.CompilerParams(**kw)


def pack_kernel(blocks, helpers, pos, choice, query, grad, sent, picker_out, *own):
    rows = query.shape[0]
    width = query.shape[1] // helpers
    center = pos[0]
    helper = pos[1]
    slots = blocks * CAPACITY
    targets = []
    matches = []
    block_ids = iota((blocks, rows), 0)
    for r in range(2):
        c = choice[r : r + 1, :]
        t = jnp.where(c < center, center - 1 - c, -1)
        targets.append(t)
        matches.append(block_ids == t)
    counts = jnp.where(matches[0], 1.0, 0.0) + jnp.where(matches[1], 1.0, 0.0)
    before = jnp.where(iota((rows, rows), 0) < iota((rows, rows), 1), 1.0, 0.0).astype(BF16)
    earlier = dot(counts.astype(BF16), before, 1, 0)
    picker = jnp.zeros((slots, rows), F32)
    places = []
    for r in range(2):
        p = jnp.sum(jnp.where(matches[r], earlier, 0.0), axis=0, keepdims=True)
        places.append(p)
        code = jnp.where(targets[r] >= 0, targets[r] * CAPACITY + p.astype(jnp.int32), -1)
        picker = picker + jnp.where(iota((slots, rows), 0) == code, 1.0, 0.0)
    picker_out[...] = picker.T.astype(BF16)
    low = picker.astype(BF16)
    for d in range(helpers):
        for n, source in enumerate((query, grad)):
            got = dot(low, source[:, d * width : (d + 1) * width], 1, 0)
            sent[:, d, :, n * width : (n + 1) * width] = got.reshape(
                blocks, CAPACITY, width
            ).astype(BF16)
    info = jnp.concatenate([t.astype(F32) for t in targets] + places, axis=1)
    info = jnp.broadcast_to(info, (INFO, info.shape[1])).astype(BF16)
    for k in range(helpers):
        cols = pl.ds(pl.multiple_of((helper ^ k) * width, width), width)
        own[k][0:rows, 0:width] = query[:, cols]
        own[k][0:rows, width : 2 * width] = grad[:, cols]
        own[k][rows : rows + INFO, :] = info


def tile_rows(own, helper, start, count, rows, cols):
    parts = [own[helper ^ g, 0:rows, cols] for g in range(start // rows, (start + count) // rows)]
    return jnp.concatenate(parts, axis=0)


def head_cols(head, heads, which):
    at = (which * heads + head) * HEAD_DIM
    return slice(at, at + HEAD_DIM)


def diagonal():
    return iota((TILE, TILE), 0) <= iota((TILE, TILE), 1)


def statistics_of(scores, products):
    highest = jnp.max(scores, axis=0, keepdims=True)
    weights = jnp.exp2(scores - highest)
    total = jnp.sum(weights, axis=0, keepdims=True)
    crossed = jnp.sum(weights * products, axis=0, keepdims=True)
    return highest + jnp.log(total) * LOG2E, crossed / total


def own_statistics_kernel(heads, helpers, pos, own, key, value, out):
    helper = pos[1]
    rows = own.shape[1] - INFO
    length = key.shape[0]
    keep = diagonal()
    for head in range(heads):
        hc = slice(head * HEAD_DIM, (head + 1) * HEAD_DIM)
        for start in range(0, length, TILE):
            end = start + TILE
            q = tile_rows(own, helper, start, TILE, rows, head_cols(head, heads, 0))
            g = tile_rows(own, helper, start, TILE, rows, head_cols(head, heads, 1))
            scores = dot(key[0:end, hc], q, 1, 1) * (SCALING * LOG2E)
            products = dot(value[0:end, hc], g, 1, 1)
            last = jnp.where(keep, scores[start:end], NEGATIVE)
            scores = jnp.concatenate([scores[0:start], last], axis=0) if start else last
            log_sum, mean = statistics_of(scores, products)
            out[2 * head : 2 * head + 1, start:end] = log_sum
            out[2 * head + 1 : 2 * head + 2, start:end] = mean
    for n in range(4):
        parts = [
            own[helper ^ g, rows : rows + INFO, n * rows : (n + 1) * rows].astype(F32)[0:1]
            for g in range(helpers)
        ]
        out[2 * heads + n : 2 * heads + n + 1, :] = jnp.concatenate(parts, axis=1)


def routed_statistics_kernel(heads, group, pos, rows, key, value, out):
    for head in range(heads):
        hc = slice(head * HEAD_DIM, (head + 1) * HEAD_DIM)
        scores = dot(key[:, hc], rows[:, head_cols(head, heads, 0)], 1, 1) * (SCALING * LOG2E)
        products = dot(value[:, hc], rows[:, head_cols(head, heads, 1)], 1, 1)
        log_sum, mean = statistics_of(scores, products)
        for a in range(TILE // group):
            cut = slice(a * group, (a + 1) * group)
            out[a, head : head + 1, 0:group] = log_sum[:, cut]
            out[a, head : head + 1, group : 2 * group] = mean[:, cut]


def combine_kernel(heads, helpers, stats, got, totals, slots):
    length = stats.shape[1]
    blocks = got.shape[0]
    group = got.shape[2] // 2
    rows = length // helpers
    exact = lax.Precision.HIGHEST
    slot = iota((group, length), 0)
    in_group = (slot // CAPACITY) == (iota((group, length), 1) // rows)
    slot_place = (slot % CAPACITY).astype(F32)
    block_ids = iota((blocks, length), 0).astype(F32)
    hots = []
    masks = []
    present = []
    for r in range(2):
        t = stats[2 * heads + r : 2 * heads + r + 1, :]
        p = stats[2 * heads + 2 + r : 2 * heads + 3 + r, :]
        present.append(t >= 0.0)
        hots.append(jnp.where(block_ids == t, 1.0, 0.0))
        masks.append(in_group & (slot_place == p) & (t >= 0.0))
    for head in range(heads):
        part = got[:, head, :]
        logs = [stats[2 * head : 2 * head + 1, :]]
        means = [stats[2 * head + 1 : 2 * head + 2, :]]
        for r in range(2):
            spread = dot(part, hots[r], 0, 0, exact)
            log_r = jnp.sum(jnp.where(masks[r], spread[0:group], 0.0), axis=0, keepdims=True)
            mean_r = jnp.sum(
                jnp.where(masks[r], spread[group : 2 * group], 0.0), axis=0, keepdims=True
            )
            logs.append(jnp.where(present[r], log_r, NEGATIVE))
            means.append(mean_r)
        top = jnp.maximum(jnp.maximum(logs[0], logs[1]), logs[2])
        shares = [jnp.exp2(v - top) for v in logs]
        norm = shares[0] + shares[1] + shares[2]
        log_total = top + jnp.log(norm) * LOG2E
        center = (shares[0] * means[0] + shares[1] * means[1] + shares[2] * means[2]) / norm
        totals[2 * head : 2 * head + 1, :] = log_total
        totals[2 * head + 1 : 2 * head + 2, :] = center
        result = jnp.zeros((blocks, 2 * group), F32)
        for r in range(2):
            both = jnp.concatenate(
                [jnp.where(masks[r], log_total, 0.0), jnp.where(masks[r], center, 0.0)], axis=0
            )
            result = result + dot(hots[r], both, 1, 1, exact)
        slots[:, head, :] = result


def own_gradients_kernel(heads, pos, own, key, value, totals, query_out, key_out, value_out):
    helper = pos[1]
    rows = own.shape[1] - INFO
    length = key.shape[0]
    keep = diagonal()
    for head in range(heads):
        hc = slice(head * HEAD_DIM, (head + 1) * HEAD_DIM)
        turned = key[:, hc].T
        for start in reversed(range(0, length, TILE)):
            end = start + TILE
            q = tile_rows(own, helper, start, TILE, rows, head_cols(head, heads, 0))
            g = tile_rows(own, helper, start, TILE, rows, head_cols(head, heads, 1))
            log_total = totals[2 * head : 2 * head + 1, start:end]
            center = totals[2 * head + 1 : 2 * head + 2, start:end]
            scores = dot(key[0:end, hc], q, 1, 1) * (SCALING * LOG2E)
            products = dot(value[0:end, hc], g, 1, 1)
            last = jnp.where(keep, scores[start:end], NEGATIVE)
            scores = jnp.concatenate([scores[0:start], last], axis=0) if start else last
            probs = jnp.exp2(scores - log_total)
            mixed = (probs * (products - center)).astype(BF16)
            value_new = dot(probs.astype(BF16), g, 1, 0)
            key_new = dot(mixed, q, 1, 0)
            if end == length:
                value_out[:, hc] = value_new
                key_out[:, hc] = key_new
            else:
                value_out[0:end, hc] += value_new
                key_out[0:end, hc] += key_new
            query_new = (dot(turned[:, 0:end], mixed, 1, 0) * SCALING).T
            for n in range(TILE // rows):
                query_out[helper ^ (start // rows + n), :, hc] = query_new[
                    n * rows : (n + 1) * rows
                ].astype(BF16)


def slot_row(slots, head, which, group):
    cut = slice(which * group, (which + 1) * group)
    return jnp.concatenate([slots[a, head : head + 1, cut] for a in range(TILE // group)], axis=1)


def routed_mixed(heads, group, head, rows, key, value, slots):
    hc = slice(head * HEAD_DIM, (head + 1) * HEAD_DIM)
    scores = dot(key[:, hc], rows[:, head_cols(head, heads, 0)], 1, 1) * (SCALING * LOG2E)
    products = dot(value[:, hc], rows[:, head_cols(head, heads, 1)], 1, 1)
    probs = jnp.exp2(scores - slot_row(slots, head, 0, group))
    mixed = (probs * (products - slot_row(slots, head, 1, group))).astype(BF16)
    return probs, mixed


def routed_query_kernel(heads, group, pos, rows, key, value, slots, out, turned):
    @pl.when(pl.program_id(0) == 0)
    def _():
        for head in range(heads):
            turned[head] = key[:, head * HEAD_DIM : (head + 1) * HEAD_DIM].T

    for head in range(heads):
        hc = slice(head * HEAD_DIM, (head + 1) * HEAD_DIM)
        _, mixed = routed_mixed(heads, group, head, rows, key, value, slots)
        out[:, hc] = (dot(turned[head], mixed, 1, 0) * SCALING).T.astype(BF16)


def routed_block_kernel(
    heads, group, helpers, pos, rows, key, value, slots, key_own, value_own, query_own, *rest
):
    pieces = rest[:helpers]
    key_acc, value_acc = rest[helpers:]
    step = pl.program_id(0)

    @pl.when(step == 0)
    def _():
        key_acc[...] = key_own[...]
        value_acc[...] = value_own[...]

    for head in range(heads):
        hc = slice(head * HEAD_DIM, (head + 1) * HEAD_DIM)
        probs, mixed = routed_mixed(heads, group, head, rows, key, value, slots)
        value_acc[:, hc] += dot(probs.astype(BF16), rows[:, head_cols(head, heads, 1)], 1, 0)
        key_acc[:, hc] += dot(mixed, rows[:, head_cols(head, heads, 0)], 1, 0)

    @pl.when(step == pl.num_programs(0) - 1)
    def _():
        width = key_acc.shape[1]
        share = key_acc.shape[0] // helpers
        for k in range(helpers):
            at = pl.ds(pl.multiple_of((pos[1] ^ k) * share, share), share)
            pieces[k][:, 0:width] = query_own[k]
            pieces[k][:, width : 2 * width] = (key_acc[at, :] * SCALING).astype(BF16)
            pieces[k][:, 2 * width : 3 * width] = value_acc[at, :].astype(BF16)


def place_kernel(helpers, pos, *refs):
    pieces = refs[:helpers]
    key_out, value_out = refs[helpers:]
    width = key_out.shape[1] // helpers
    for k in range(helpers):
        cols = pl.ds(pl.multiple_of((pos[1] ^ k) * width, width), width)
        key_out[:, cols] = pieces[k][:, width : 2 * width]
        value_out[:, cols] = pieces[k][:, 2 * width : 3 * width]


def finish_kernel(helpers, pos, picker, returned, *refs):
    pieces = refs[:helpers]
    out = refs[helpers]
    width = out.shape[1] // helpers
    slots = picker.shape[1]
    for k in range(helpers):
        d = pos[1] ^ k
        cols = pl.ds(pl.multiple_of(d * width, width), width)
        terms = returned[:, d].astype(F32).reshape(slots, width).astype(BF16)
        out[:, cols] = (dot(picker[...], terms, 1, 0) + pieces[k][:, 0:width].astype(F32)).astype(
            BF16
        )


def exchange(pieces, helpers):
    received = [pieces[0]]
    for k in range(1, helpers):
        received.append(lax.ppermute(pieces[k], "help", [(i, i ^ k) for i in range(helpers)]))
    return received


def whole(shape):
    return pl.BlockSpec(shape, lambda *_: (0,) * len(shape))


def per_device(query_rows, key_rows, value_rows, output_grad, block_choice):
    blocks = lax.axis_size("ctx")
    helpers = lax.axis_size("help")
    position = jnp.stack([lax.axis_index("ctx"), lax.axis_index("help")]).astype(jnp.int32)
    _, rows, features = query_rows.shape
    length = key_rows.shape[1]
    width = features // helpers
    heads = width // HEAD_DIM
    group = helpers * CAPACITY
    slots = blocks * CAPACITY
    total = blocks * group
    steps = total // TILE
    query, grad = query_rows[0], output_grad[0]
    key, value = key_rows[0], value_rows[0]
    choice = jnp.transpose(block_choice[0])
    shape = jax.ShapeDtypeStruct

    def call(kernel, out_shape, in_specs, out_specs, grid=(1,), scratch=(), name=None):
        return pl.pallas_call(
            kernel,
            out_shape=out_shape,
            grid_spec=pltpu.PrefetchScalarGridSpec(
                num_scalar_prefetch=1,
                grid=grid,
                in_specs=in_specs,
                out_specs=out_specs,
                scratch_shapes=scratch,
            ),
            name=name,
        )

    piece = shape((rows + INFO, 2 * width), BF16)
    packed = call(
        functools.partial(pack_kernel, blocks, helpers),
        [
            shape((blocks, helpers, CAPACITY, 2 * width), BF16),
            shape((rows, slots), BF16),
        ]
        + [piece] * helpers,
        [whole((2, rows)), whole((rows, features)), whole((rows, features))],
        [whole((blocks, helpers, CAPACITY, 2 * width)), whole((rows, slots))]
        + [whole(piece.shape)] * helpers,
        name="pack",
    )(position, choice, query, grad)
    sent, picker, pieces = packed[0], packed[1], packed[2:]

    own = jnp.stack(exchange(pieces, helpers))
    with jax.named_scope("dispatch"):
        routed = lax.all_to_all(
            sent.reshape(blocks * helpers, CAPACITY, 2 * width),
            ("ctx", "help"),
            split_axis=0,
            concat_axis=0,
            tiled=True,
        ).reshape(total, 2 * width)

    block_spec = pl.BlockSpec((length, width), lambda i, pos: (0, pos[1]))
    own_spec = whole((helpers, rows + INFO, 2 * width))
    stats = call(
        functools.partial(own_statistics_kernel, heads, helpers),
        shape((2 * heads + 4, length), F32),
        [own_spec, block_spec, block_spec],
        whole((2 * heads + 4, length)),
        name="own_statistics",
    )(position, own, key, value)

    row_spec = pl.BlockSpec((TILE, 2 * width), lambda i, pos: (i, 0))
    slot_spec = pl.BlockSpec((TILE // group, heads, 2 * group), lambda i, pos: (i, 0, 0))
    slot_shape = shape((blocks, heads, 2 * group), F32)
    parts = call(
        functools.partial(routed_statistics_kernel, heads, group),
        slot_shape,
        [row_spec, block_spec, block_spec],
        slot_spec,
        grid=(steps,),
        name="routed_statistics",
    )(position, routed, key, value)
    with jax.named_scope("parts"):
        parts = lax.all_to_all(parts, "ctx", split_axis=0, concat_axis=0, tiled=True)

    totals, spread = pl.pallas_call(
        functools.partial(combine_kernel, heads, helpers),
        out_shape=[shape((2 * heads, length), F32), slot_shape],
        name="combine",
    )(stats, parts)
    with jax.named_scope("totals"):
        spread = lax.all_to_all(spread, "ctx", split_axis=0, concat_axis=0, tiled=True)

    query_own, key_own, value_own = call(
        functools.partial(own_gradients_kernel, heads),
        [shape((helpers, rows, width), BF16), shape((length, width), F32), shape((length, width), F32)],
        [own_spec, block_spec, block_spec, whole((2 * heads, length))],
        [whole((helpers, rows, width)), whole((length, width)), whole((length, width))],
        name="own_gradients",
    )(position, own, key, value, totals)

    terms = call(
        functools.partial(routed_query_kernel, heads, group),
        shape((total, width), BF16),
        [row_spec, block_spec, block_spec, slot_spec],
        pl.BlockSpec((TILE, width), lambda i, pos: (i, 0)),
        grid=(steps,),
        scratch=[pltpu.VMEM((heads, HEAD_DIM, length), BF16)],
        name="routed_query",
    )(position, routed, key, value, spread)
    with jax.named_scope("back"):
        returned = lax.all_to_all(
            terms.reshape(blocks * helpers, CAPACITY, width),
            ("ctx", "help"),
            split_axis=0,
            concat_axis=0,
            tiled=True,
        ).reshape(blocks, helpers, CAPACITY, width)

    share = length // helpers
    piece = shape((share, 3 * width), BF16)
    pieces = call(
        functools.partial(routed_block_kernel, heads, group, helpers),
        [piece] * helpers,
        [
            row_spec,
            block_spec,
            block_spec,
            slot_spec,
            whole((length, width)),
            whole((length, width)),
            whole((helpers, rows, width)),
        ],
        [whole(piece.shape)] * helpers,
        grid=(steps,),
        scratch=[pltpu.VMEM((length, width), F32), pltpu.VMEM((length, width), F32)],
        name="routed_block",
    )(position, routed, key, value, spread, key_own, value_own, query_own)
    pieces = exchange(pieces, helpers)

    key_grad, value_grad = call(
        functools.partial(place_kernel, helpers),
        [shape((share, features), BF16)] * 2,
        [whole(piece.shape)] * helpers,
        [whole((share, features))] * 2,
        name="place",
    )(position, *pieces)
    query_grad = call(
        functools.partial(finish_kernel, helpers),
        shape((rows, features), BF16),
        [whole((rows, slots)), whole((blocks, helpers, CAPACITY, width))]
        + [whole(piece.shape)] * helpers,
        whole((rows, features)),
        name="finish",
    )(position, picker, returned, *pieces)
    return query_grad[None], key_grad[None], value_grad[None]


def solution(mesh):
    split = P(None, ("ctx", "help"), None)
    shared = P(None, "ctx", None)
    return jax.shard_map(
        per_device,
        mesh=mesh,
        in_specs=(split, shared, shared, split, split),
        out_specs=(split, split, split),
        check_vma=False,
    )
```

```python
import functools

import jax
import jax.numpy as jnp
from jax import lax
from jax.experimental import pallas as pl
from jax.experimental.pallas import tpu as pltpu
from jax.sharding import PartitionSpec as P

HEAD_DIM = 128
CAPACITY = 8
NEGATIVE = -1e30
LOG2E = 1.4426950408889634
LN2 = 0.6931471805599453
SCALING = HEAD_DIM ** (-0.5)
INFO = 16
TILE = 256
CHUNK = 64
F32 = jnp.float32
BF16 = jnp.bfloat16


def iota(shape, dim):
    return lax.broadcasted_iota(jnp.int32, shape, dim)


def dot(a, b, ca, cb, precision=None):
    return lax.dot_general(
        a, b, (((ca,), (cb,)), ((), ())), precision=precision, preferred_element_type=F32
    )


def params(**kw):
    return pltpu.CompilerParams(**kw)


def pack_kernel(blocks, helpers, pos, choice, query, grad, sent, picker_out, *own):
    rows = query.shape[0]
    width = query.shape[1] // helpers
    center = pos[0]
    helper = pos[1]
    slots = blocks * CAPACITY
    targets = []
    matches = []
    block_ids = iota((blocks, rows), 0)
    for r in range(2):
        c = choice[r : r + 1, :]
        t = jnp.where(c < center, center - 1 - c, -1)
        targets.append(t)
        matches.append(block_ids == t)
    counts = jnp.where(matches[0], 1.0, 0.0) + jnp.where(matches[1], 1.0, 0.0)
    before = jnp.where(iota((rows, rows), 0) < iota((rows, rows), 1), 1.0, 0.0).astype(BF16)
    earlier = dot(counts.astype(BF16), before, 1, 0)
    picker = jnp.zeros((slots, rows), F32)
    places = []
    for r in range(2):
        p = jnp.sum(jnp.where(matches[r], earlier, 0.0), axis=0, keepdims=True)
        places.append(p)
        code = jnp.where(targets[r] >= 0, targets[r] * CAPACITY + p.astype(jnp.int32), -1)
        picker = picker + jnp.where(iota((slots, rows), 0) == code, 1.0, 0.0)
    picker_out[...] = picker.T.astype(BF16)
    low = picker.astype(BF16)
    for d in range(helpers):
        for n, source in enumerate((query, grad)):
            got = dot(low, source[:, d * width : (d + 1) * width], 1, 0)
            sent[d, :, :, n * width : (n + 1) * width] = got.reshape(
                blocks, CAPACITY, width
            ).astype(BF16)
    info = jnp.concatenate([t.astype(F32) for t in targets] + places, axis=1)
    info = jnp.broadcast_to(info, (INFO, info.shape[1])).astype(BF16)
    for k in range(helpers):
        cols = pl.ds(pl.multiple_of((helper ^ k) * width, width), width)
        own[k][0:rows, 0:width] = query[:, cols]
        own[k][0:rows, width : 2 * width] = grad[:, cols]
        own[k][rows : rows + INFO, :] = info


def head_cols(head, heads, which):
    at = (which * heads + head) * HEAD_DIM
    return slice(at, at + HEAD_DIM)


def cols_of(head):
    return slice(head * HEAD_DIM, (head + 1) * HEAD_DIM)


def own_tile(own, helper, start, rows, cols):
    parts = [own[helper ^ g, 0:rows, cols] for g in range(start // rows, (start + TILE) // rows)]
    return jnp.concatenate(parts, axis=0)


def routed_tile(routed, tile, cols):
    helpers, _, capacity, _ = routed.shape
    group = helpers * capacity
    count = TILE // group
    parts = [
        routed[:, tile * count + a, :, cols].astype(F32).reshape(group, HEAD_DIM)
        for a in range(count)
    ]
    return jnp.concatenate(parts, axis=0).astype(BF16)


def statistics_of(key, value, q, g, masked_from):
    scores = dot(key, q, 1, 1)
    products = dot(value, g, 1, 1)
    shape = (8, q.shape[0])
    highest = jnp.full(shape, NEGATIVE, F32)
    total = jnp.zeros(shape, F32)
    crossed = jnp.zeros(shape, F32)
    for at in range(0, key.shape[0], CHUNK):
        part = scores[at : at + CHUNK] * (SCALING * LOG2E)
        if masked_from is not None and at + CHUNK > masked_from:
            keep = iota(part.shape, 0) + (at - masked_from) <= iota(part.shape, 1)
            part = jnp.where(keep, part, NEGATIVE)
        part = part.reshape((CHUNK // 8,) + shape)
        newer = jnp.maximum(highest, jnp.max(part, axis=0))
        weights = jnp.exp2(part - newer)
        if masked_from is not None and at + CHUNK > masked_from:
            weights = jnp.where(keep.reshape(weights.shape), weights, 0.0)
        shrink = jnp.exp2(highest - newer)
        total = total * shrink + jnp.sum(weights, axis=0)
        crossed = crossed * shrink + jnp.sum(
            weights * products[at : at + CHUNK].reshape(part.shape), axis=0
        )
        highest = newer
    top = jnp.max(highest, axis=0, keepdims=True)
    shrink = jnp.exp2(highest - top)
    total = jnp.sum(total * shrink, axis=0, keepdims=True)
    crossed = jnp.sum(crossed * shrink, axis=0, keepdims=True)
    return top + jnp.log(total) * LOG2E, crossed / total


def own_statistics_kernel(heads, helpers, pos, own, key, value, out):
    helper = pos[1]
    rows = own.shape[1] - INFO
    length = key.shape[0]
    for head in range(heads):
        hc = cols_of(head)
        for start in range(0, length, TILE):
            end = start + TILE
            q = own_tile(own, helper, start, rows, head_cols(head, heads, 0))
            g = own_tile(own, helper, start, rows, head_cols(head, heads, 1))
            log_sum, mean = statistics_of(key[0:end, hc], value[0:end, hc], q, g, start)
            out[2 * head : 2 * head + 1, start:end] = log_sum
            out[2 * head + 1 : 2 * head + 2, start:end] = mean
    for n in range(4):
        parts = [
            own[helper ^ g, rows : rows + INFO, n * rows : (n + 1) * rows].astype(F32)[0:1]
            for g in range(helpers)
        ]
        out[2 * heads + n : 2 * heads + n + 1, :] = jnp.concatenate(parts, axis=1)


def routed_statistics_kernel(heads, routed, key, value, out):
    helpers, blocks, capacity, _ = routed.shape
    group = helpers * capacity
    count = TILE // group

    def body(tile, _):
        for head in range(heads):
            hc = cols_of(head)
            q = routed_tile(routed, tile, head_cols(head, heads, 0))
            g = routed_tile(routed, tile, head_cols(head, heads, 1))
            log_sum, mean = statistics_of(key[:, hc], value[:, hc], q, g, None)
            for a in range(count):
                cut = slice(a * group, (a + 1) * group)
                out[tile * count + a, head : head + 1, 0:group] = log_sum[:, cut]
                out[tile * count + a, head : head + 1, group : 2 * group] = mean[:, cut]
        return 0

    lax.fori_loop(0, blocks // count, body, 0)


def thirds(x, axis):
    high = x.astype(BF16)
    rest = x - high.astype(F32)
    middle = rest.astype(BF16)
    low = (rest - middle.astype(F32)).astype(BF16)
    return jnp.concatenate([high, middle, low], axis=axis)


def combine_kernel(heads, helpers, stats, got, totals, slots):
    length = stats.shape[1]
    blocks = got.shape[0]
    group = got.shape[2] // 2
    rows = length // helpers
    wide = 2 * group
    slot = iota((group, length), 0)
    in_group = (slot // CAPACITY) == (iota((group, length), 1) // rows)
    slot_place = (slot % CAPACITY).astype(F32)
    block_ids = iota((blocks, length), 0).astype(F32)
    hots = []
    masks = []
    present = []
    for r in range(2):
        t = stats[2 * heads + r : 2 * heads + r + 1, :]
        p = stats[2 * heads + 2 + r : 2 * heads + 3 + r, :]
        present.append(t >= 0.0)
        hots.append(jnp.where(block_ids == t, 1.0, 0.0).astype(BF16))
        masks.append(in_group & (slot_place == p) & (t >= 0.0))
    for head in range(heads):
        part = thirds(got[:, head, :].T, 1)
        logs = [stats[2 * head : 2 * head + 1, :]]
        means = [stats[2 * head + 1 : 2 * head + 2, :]]
        for r in range(2):
            hot = jnp.concatenate([hots[r]] * 3, axis=0)
            spread = dot(part, hot, 1, 0)
            log_r = jnp.sum(jnp.where(masks[r], spread[0:group], 0.0), axis=0, keepdims=True)
            mean_r = jnp.sum(jnp.where(masks[r], spread[group:wide], 0.0), axis=0, keepdims=True)
            logs.append(jnp.where(present[r], log_r, NEGATIVE))
            means.append(mean_r)
        top = jnp.maximum(jnp.maximum(logs[0], logs[1]), logs[2])
        shares = [jnp.exp2(v - top) for v in logs]
        norm = shares[0] + shares[1] + shares[2]
        log_total = top + jnp.log(norm) * LOG2E
        center = (shares[0] * means[0] + shares[1] * means[1] + shares[2] * means[2]) / norm
        totals[2 * head : 2 * head + 1, :] = log_total
        totals[2 * head + 1 : 2 * head + 2, :] = center
        logs3 = thirds(log_total, 0).astype(F32)
        means3 = thirds(center, 0).astype(F32)
        result = jnp.zeros((blocks, wide), F32)
        for r in range(2):
            for n in range(3):
                both = jnp.concatenate(
                    [
                        jnp.where(masks[r], logs3[n : n + 1], 0.0),
                        jnp.where(masks[r], means3[n : n + 1], 0.0),
                    ],
                    axis=0,
                ).astype(BF16)
                result = result + dot(hots[r], both, 1, 1)
        slots[:, head, :] = result


def mixed_into(mixed, probs, key, value, q, g, log_total, center, masked_from):
    scores = dot(key, q, 1, 1)
    products = dot(value, g, 1, 1)
    for at in range(0, key.shape[0], CHUNK):
        rows = slice(at, at + CHUNK)
        part = scores[rows] * (SCALING * LOG2E)
        if masked_from is not None and at + CHUNK > masked_from:
            keep = iota(part.shape, 0) + (at - masked_from) <= iota(part.shape, 1)
            part = jnp.where(keep, part, NEGATIVE)
        weights = jnp.exp2(part - log_total)
        if probs is not None:
            probs[rows, :] = weights.astype(BF16)
        mixed[rows, :] = (weights * (products[rows] - center)).astype(BF16)


def own_gradients_kernel(
    heads, pos, own, key, value, totals, query_out, key_out, value_out, mixed, probs
):
    helper = pos[1]
    rows = own.shape[1] - INFO
    length = key.shape[0]
    for head in range(heads):
        hc = cols_of(head)
        turned = key[:, hc].T
        for start in reversed(range(0, length, TILE)):
            end = start + TILE
            q = own_tile(own, helper, start, rows, head_cols(head, heads, 0))
            g = own_tile(own, helper, start, rows, head_cols(head, heads, 1))
            log_total = totals[2 * head : 2 * head + 1, start:end]
            center = totals[2 * head + 1 : 2 * head + 2, start:end]
            mixed_into(
                mixed, probs, key[0:end, hc], value[0:end, hc], q, g, log_total, center, start
            )
            value_new = dot(probs[0:end, :], g, 1, 0)
            key_new = dot(mixed[0:end, :], q, 1, 0)
            if end == length:
                value_out[:, hc] = value_new
                key_out[:, hc] = key_new
            else:
                value_out[0:end, hc] += value_new
                key_out[0:end, hc] += key_new
            query_new = (dot(turned[:, 0:end], mixed[0:end, :], 1, 0) * SCALING).T
            for n in range(TILE // rows):
                query_out[helper ^ (start // rows + n), :, hc] = query_new[
                    n * rows : (n + 1) * rows
                ].astype(BF16)


def slot_row(slots, tile, head, which, group):
    cut = slice(which * group, (which + 1) * group)
    count = TILE // group
    return jnp.concatenate(
        [slots[tile * count + a, head : head + 1, cut] for a in range(count)], axis=1
    )


def routed_query_kernel(heads, routed, key, value, slots, out, mixed):
    helpers, blocks, capacity, _ = routed.shape
    group = helpers * capacity
    count = TILE // group
    turned = [key[:, cols_of(head)].T for head in range(heads)]

    def body(tile, _):
        for head in range(heads):
            hc = cols_of(head)
            q = routed_tile(routed, tile, head_cols(head, heads, 0))
            g = routed_tile(routed, tile, head_cols(head, heads, 1))
            log_total = slot_row(slots, tile, head, 0, group)
            center = slot_row(slots, tile, head, 1, group)
            mixed_into(
                mixed.at[head], None, key[:, hc], value[:, hc], q, g, log_total, center, None
            )
            query_new = (dot(turned[head], mixed[head], 1, 0) * SCALING).T
            for a in range(count):
                out[:, tile * count + a, :, hc] = (
                    query_new[a * group : (a + 1) * group]
                    .reshape(helpers, capacity, HEAD_DIM)
                    .astype(BF16)
                )
        return 0

    lax.fori_loop(0, blocks // count, body, 0)


def routed_block_kernel(
    heads, helpers, pos, routed, key, value, slots, key_own, value_own, query_own, *rest
):
    pieces = rest[:helpers]
    key_acc, value_acc, mixed, probs = rest[helpers:]
    _, blocks, capacity, _ = routed.shape
    group = helpers * capacity
    key_acc[...] = key_own[...]
    value_acc[...] = value_own[...]

    def body(tile, _):
        for head in range(heads):
            hc = cols_of(head)
            q = routed_tile(routed, tile, head_cols(head, heads, 0))
            g = routed_tile(routed, tile, head_cols(head, heads, 1))
            log_total = slot_row(slots, tile, head, 0, group)
            center = slot_row(slots, tile, head, 1, group)
            mixed_into(
                mixed.at[head],
                probs.at[head],
                key[:, hc],
                value[:, hc],
                q,
                g,
                log_total,
                center,
                None,
            )
            value_acc[:, hc] += dot(probs[head], g, 1, 0)
            key_acc[:, hc] += dot(mixed[head], q, 1, 0)
        return 0

    lax.fori_loop(0, blocks * group // TILE, body, 0)
    width = key_acc.shape[1]
    share = key_acc.shape[0] // helpers
    for k in range(helpers):
        at = pl.ds(pl.multiple_of((pos[1] ^ k) * share, share), share)
        pieces[k][:, 0:width] = query_own[k]
        pieces[k][:, width : 2 * width] = (key_acc[at, :] * SCALING).astype(BF16)
        pieces[k][:, 2 * width : 3 * width] = value_acc[at, :].astype(BF16)


def place_kernel(helpers, pos, *refs):
    pieces = refs[:helpers]
    key_out, value_out = refs[helpers:]
    width = key_out.shape[1] // helpers
    for k in range(helpers):
        cols = pl.ds(pl.multiple_of((pos[1] ^ k) * width, width), width)
        key_out[:, cols] = pieces[k][:, width : 2 * width]
        value_out[:, cols] = pieces[k][:, 2 * width : 3 * width]


def finish_kernel(helpers, pos, picker, returned, *refs):
    pieces = refs[:helpers]
    out = refs[helpers]
    width = out.shape[1] // helpers
    slots = picker.shape[1]
    for k in range(helpers):
        d = pos[1] ^ k
        cols = pl.ds(pl.multiple_of(d * width, width), width)
        terms = returned[d].astype(F32).reshape(slots, width).astype(BF16)
        out[:, cols] = (dot(picker[...], terms, 1, 0) + pieces[k][:, 0:width].astype(F32)).astype(
            BF16
        )


def exchange(pieces, helpers):
    received = [pieces[0]]
    for k in range(1, helpers):
        received.append(lax.ppermute(pieces[k], "help", [(i, i ^ k) for i in range(helpers)]))
    return received


def call(kernel, out_shape, name, scratch=()):
    return pl.pallas_call(kernel, out_shape=out_shape, scratch_shapes=scratch, name=name)


def with_position(kernel, out_shape, name, operands, scratch=()):
    vmem = pl.BlockSpec(memory_space=pltpu.VMEM)
    return pl.pallas_call(
        kernel,
        out_shape=out_shape,
        in_specs=[pl.BlockSpec(memory_space=pltpu.SMEM)] + [vmem] * operands,
        scratch_shapes=scratch,
        name=name,
    )


def swap(array, axes):
    return lax.all_to_all(array, axes, split_axis=0, concat_axis=0, tiled=True)


def per_device(query_rows, key_rows, value_rows, output_grad, block_choice):
    blocks = lax.axis_size("ctx")
    helpers = lax.axis_size("help")
    helper = lax.axis_index("help")
    position = jnp.stack([lax.axis_index("ctx"), helper]).astype(jnp.int32)
    _, rows, features = query_rows.shape
    length = key_rows.shape[1]
    width = features // helpers
    heads = width // HEAD_DIM
    group = helpers * CAPACITY
    slots = blocks * CAPACITY
    shape = jax.ShapeDtypeStruct
    everyone = ("help", "ctx")

    piece = shape((rows + INFO, 2 * width), BF16)
    packed = with_position(
        functools.partial(pack_kernel, blocks, helpers),
        [
            shape((helpers, blocks, CAPACITY, 2 * width), BF16),
            shape((rows, slots), BF16),
        ]
        + [piece] * helpers,
        "pack",
        3,
    )(position, jnp.transpose(block_choice[0]), query_rows[0], output_grad[0])
    sent, picker, pieces = packed[0], packed[1], packed[2:]

    own = jnp.stack(exchange(pieces, helpers))
    with jax.named_scope("dispatch"):
        routed = swap(sent.reshape(blocks * helpers, CAPACITY, 2 * width), everyone)
    routed = routed.reshape(helpers, blocks, CAPACITY, 2 * width)

    key = lax.dynamic_slice_in_dim(key_rows[0], helper * width, width, 1)
    value = lax.dynamic_slice_in_dim(value_rows[0], helper * width, width, 1)
    stats = with_position(
        functools.partial(own_statistics_kernel, heads, helpers),
        shape((2 * heads + 4, length), F32),
        "own_statistics",
        3,
    )(position, own, key, value)

    slot_shape = shape((blocks, heads, 2 * group), F32)
    parts = call(
        functools.partial(routed_statistics_kernel, heads), slot_shape, "routed_statistics"
    )(routed, key, value)
    with jax.named_scope("parts"):
        parts = swap(parts, "ctx")

    totals, spread = call(
        functools.partial(combine_kernel, heads, helpers),
        [shape((2 * heads, length), F32), slot_shape],
        "combine",
    )(stats, parts)
    with jax.named_scope("totals"):
        spread = swap(spread, "ctx")

    tile = (heads, length, TILE)
    query_own, key_own, value_own = with_position(
        functools.partial(own_gradients_kernel, heads),
        [
            shape((helpers, rows, width), BF16),
            shape((length, width), F32),
            shape((length, width), F32),
        ],
        "own_gradients",
        4,
        [pltpu.VMEM(tile[1:], BF16), pltpu.VMEM(tile[1:], BF16)],
    )(position, own, key, value, totals)
    spread, query_own, key_own, value_own = lax.optimization_barrier(
        (spread, query_own, key_own, value_own)
    )

    terms = call(
        functools.partial(routed_query_kernel, heads),
        shape((helpers, blocks, CAPACITY, width), BF16),
        "routed_query",
        [pltpu.VMEM(tile, BF16)],
    )(routed, key, value, spread)
    with jax.named_scope("back"):
        returned = swap(terms.reshape(blocks * helpers, CAPACITY, width), everyone)
    returned = returned.reshape(helpers, blocks, CAPACITY, width)

    share = length // helpers
    pieces = with_position(
        functools.partial(routed_block_kernel, heads, helpers),
        [shape((share, 3 * width), BF16)] * helpers,
        "routed_block",
        7,
        [pltpu.VMEM((length, width), F32)] * 2 + [pltpu.VMEM(tile, BF16)] * 2,
    )(position, routed, key, value, spread, key_own, value_own, query_own)
    pieces = exchange(pieces, helpers)

    key_grad, value_grad = with_position(
        functools.partial(place_kernel, helpers),
        [shape((share, features), BF16)] * 2,
        "place",
        helpers,
    )(position, *pieces)
    query_grad = with_position(
        functools.partial(finish_kernel, helpers),
        shape((rows, features), BF16),
        "finish",
        helpers + 2,
    )(position, picker, returned, *pieces)
    return query_grad[None], key_grad[None], value_grad[None]


def solution(mesh):
    split = P(None, ("ctx", "help"), None)
    shared = P(None, "ctx", None)
    return jax.shard_map(
        per_device,
        mesh=mesh,
        in_specs=(split, shared, shared, split, split),
        out_specs=(split, split, split),
        check_vma=False,
    )
```

```python
import functools

import jax
import jax.numpy as jnp
from jax import lax
from jax.experimental import pallas as pl
from jax.experimental.pallas import tpu as pltpu
from jax.sharding import PartitionSpec as P


HEAD_DIM = 128
CAPACITY = 8
NEGATIVE = -1e30
LOG2E = 1.4426950408889634
SCALING = HEAD_DIM ** (-0.5)
INFO = 16
TILE = 256
CHUNK = 64
STRIP = 256
VMEM_BYTES = 24 * 2**20
F32 = jnp.float32
BF16 = jnp.bfloat16


def iota(shape, dim):
    return lax.broadcasted_iota(jnp.int32, shape, dim)


def dot(a, b, ca, cb, precision=None):
    return lax.dot_general(
        a, b, (((ca,), (cb,)), ((), ())), precision=precision, preferred_element_type=F32
    )


def pack_kernel(blocks, helpers, pos, choice, query, grad, sent, picker_out, *own):
    rows = query.shape[0]
    width = query.shape[1] // helpers
    center = pos[0]
    helper = pos[1]
    slots = blocks * CAPACITY
    targets = []
    matches = []
    block_ids = iota((blocks, rows), 0)
    for r in range(2):
        c = choice[r : r + 1, :]
        t = jnp.where(c < center, center - 1 - c, -1)
        targets.append(t)
        matches.append(block_ids == t)
    counts = jnp.where(matches[0], 1.0, 0.0) + jnp.where(matches[1], 1.0, 0.0)
    before = jnp.where(iota((rows, rows), 0) < iota((rows, rows), 1), 1.0, 0.0).astype(BF16)
    earlier = dot(counts.astype(BF16), before, 1, 0)
    picker = jnp.zeros((slots, rows), F32)
    places = []
    for r in range(2):
        p = jnp.sum(jnp.where(matches[r], earlier, 0.0), axis=0, keepdims=True)
        places.append(p)
        code = jnp.where(targets[r] >= 0, targets[r] * CAPACITY + p.astype(jnp.int32), -1)
        picker = picker + jnp.where(iota((slots, rows), 0) == code, 1.0, 0.0)
    picker_out[...] = picker.T.astype(BF16)
    low = picker.astype(BF16)
    for d in range(helpers):
        for n, source in enumerate((query, grad)):
            got = dot(low, source[:, d * width : (d + 1) * width], 1, 0)
            sent[d, :, :, n * width : (n + 1) * width] = got.reshape(
                blocks, CAPACITY, width
            ).astype(BF16)
    info = jnp.concatenate([t.astype(F32) for t in targets] + places, axis=1)
    info = jnp.broadcast_to(info, (INFO, info.shape[1])).astype(BF16)
    for k in range(helpers):
        cols = pl.ds(pl.multiple_of((helper ^ k) * width, width), width)
        piece = piece_ref(own, k)
        piece[0:rows, 0:width] = query[:, cols]
        piece[0:rows, width : 2 * width] = grad[:, cols]
        piece[rows : rows + INFO, :] = info


def head_cols(head, heads, which):
    at = (which * heads + head) * HEAD_DIM
    return slice(at, at + HEAD_DIM)


def cols_of(head):
    return slice(head * HEAD_DIM, (head + 1) * HEAD_DIM)


def own_tile(own, helper, start, rows, cols):
    parts = [own[helper ^ g, 0:rows, cols] for g in range(start // rows, (start + TILE) // rows)]
    return jnp.concatenate(parts, axis=0)


def routed_tile(routed, tile, cols):
    helpers, _, capacity, _ = routed.shape
    group = helpers * capacity
    count = TILE // group
    parts = [
        routed[:, tile * count + a, :, cols].astype(F32).reshape(group, HEAD_DIM)
        for a in range(count)
    ]
    return jnp.concatenate(parts, axis=0).astype(BF16)


def statistics_of(key, value, q, g, masked_from):
    scores = dot(key, q, 1, 1)
    products = dot(value, g, 1, 1)
    shape = (8, q.shape[0])
    highest = jnp.full(shape, NEGATIVE, F32)
    total = jnp.zeros(shape, F32)
    crossed = jnp.zeros(shape, F32)
    for at in range(0, key.shape[0], CHUNK):
        part = scores[at : at + CHUNK] * (SCALING * LOG2E)
        if masked_from is not None and at + CHUNK > masked_from:
            keep = iota(part.shape, 0) + (at - masked_from) <= iota(part.shape, 1)
            part = jnp.where(keep, part, NEGATIVE)
        part = part.reshape((CHUNK // 8,) + shape)
        newer = jnp.maximum(highest, jnp.max(part, axis=0))
        weights = jnp.exp2(part - newer)
        if masked_from is not None and at + CHUNK > masked_from:
            weights = jnp.where(keep.reshape(weights.shape), weights, 0.0)
        shrink = jnp.exp2(highest - newer)
        total = total * shrink + jnp.sum(weights, axis=0)
        crossed = crossed * shrink + jnp.sum(
            weights * products[at : at + CHUNK].reshape(part.shape), axis=0
        )
        highest = newer
    top = jnp.max(highest, axis=0, keepdims=True)
    shrink = jnp.exp2(highest - top)
    total = jnp.sum(total * shrink, axis=0, keepdims=True)
    crossed = jnp.sum(crossed * shrink, axis=0, keepdims=True)
    return top + jnp.log(total) * LOG2E, crossed / total


def own_statistics_kernel(heads, helpers, pos, own, key, value, out):
    helper = pos[1]
    rows = own.shape[1] - INFO
    length = key.shape[0]
    for head in range(heads):
        hc = cols_of(head)
        for start in range(0, length, TILE):
            end = start + TILE
            q = own_tile(own, helper, start, rows, head_cols(head, heads, 0))
            g = own_tile(own, helper, start, rows, head_cols(head, heads, 1))
            log_sum, mean = statistics_of(key[0:end, hc], value[0:end, hc], q, g, start)
            out[2 * head : 2 * head + 1, start:end] = log_sum
            out[2 * head + 1 : 2 * head + 2, start:end] = mean
    for n in range(4):
        parts = [
            own[helper ^ g, rows : rows + INFO, n * rows : (n + 1) * rows].astype(F32)[0:1]
            for g in range(helpers)
        ]
        out[2 * heads + n : 2 * heads + n + 1, :] = jnp.concatenate(parts, axis=1)


def routed_statistics_kernel(heads, routed, key, value, out):
    helpers, blocks, capacity, _ = routed.shape
    group = helpers * capacity
    count = TILE // group

    def body(tile, _):
        for head in range(heads):
            hc = cols_of(head)
            q = routed_tile(routed, tile, head_cols(head, heads, 0))
            g = routed_tile(routed, tile, head_cols(head, heads, 1))
            log_sum, mean = statistics_of(key[:, hc], value[:, hc], q, g, None)
            for a in range(count):
                cut = slice(a * group, (a + 1) * group)
                out[tile * count + a, head : head + 1, 0:group] = log_sum[:, cut]
                out[tile * count + a, head : head + 1, group : 2 * group] = mean[:, cut]
        return 0

    lax.fori_loop(0, blocks // count, body, 0)


def thirds(x, axis):
    high = x.astype(BF16)
    rest = x - high.astype(F32)
    middle = rest.astype(BF16)
    low = (rest - middle.astype(F32)).astype(BF16)
    return jnp.concatenate([high, middle, low], axis=axis)


def combine_kernel(heads, helpers, stats, got, totals, slots):
    length = stats.shape[1]
    blocks = got.shape[0]
    group = got.shape[2] // 2
    rows = length // helpers
    wide = 2 * group
    slot = iota((group, length), 0)
    in_group = (slot // CAPACITY) == (iota((group, length), 1) // rows)
    slot_place = (slot % CAPACITY).astype(F32)
    block_ids = iota((blocks, length), 0).astype(F32)
    hots = []
    masks = []
    present = []
    for r in range(2):
        t = stats[2 * heads + r : 2 * heads + r + 1, :]
        p = stats[2 * heads + 2 + r : 2 * heads + 3 + r, :]
        present.append(t >= 0.0)
        hots.append(jnp.where(block_ids == t, 1.0, 0.0).astype(BF16))
        masks.append(in_group & (slot_place == p) & (t >= 0.0))
    for head in range(heads):
        part = thirds(got[:, head, :].T, 1)
        logs = [stats[2 * head : 2 * head + 1, :]]
        means = [stats[2 * head + 1 : 2 * head + 2, :]]
        for r in range(2):
            hot = jnp.concatenate([hots[r]] * 3, axis=0)
            spread = dot(part, hot, 1, 0)
            log_r = jnp.sum(jnp.where(masks[r], spread[0:group], 0.0), axis=0, keepdims=True)
            mean_r = jnp.sum(jnp.where(masks[r], spread[group:wide], 0.0), axis=0, keepdims=True)
            logs.append(jnp.where(present[r], log_r, NEGATIVE))
            means.append(mean_r)
        top = jnp.maximum(jnp.maximum(logs[0], logs[1]), logs[2])
        shares = [jnp.exp2(v - top) for v in logs]
        norm = shares[0] + shares[1] + shares[2]
        log_total = top + jnp.log(norm) * LOG2E
        center = (shares[0] * means[0] + shares[1] * means[1] + shares[2] * means[2]) / norm
        totals[2 * head : 2 * head + 1, :] = log_total
        totals[2 * head + 1 : 2 * head + 2, :] = center
        logs3 = thirds(log_total, 0).astype(F32)
        means3 = thirds(center, 0).astype(F32)
        result = jnp.zeros((blocks, wide), F32)
        for r in range(2):
            for n in range(3):
                both = jnp.concatenate(
                    [
                        jnp.where(masks[r], logs3[n : n + 1], 0.0),
                        jnp.where(masks[r], means3[n : n + 1], 0.0),
                    ],
                    axis=0,
                ).astype(BF16)
                result = result + dot(hots[r], both, 1, 1)
        slots[:, head, :] = result


def mixed_into(mixed, probs, key, value, q, g, log_total, center, masked_from):
    scores = dot(key, q, 1, 1)
    products = dot(value, g, 1, 1)
    for at in range(0, key.shape[0], CHUNK):
        rows = slice(at, at + CHUNK)
        part = scores[rows] * (SCALING * LOG2E)
        if masked_from is not None and at + CHUNK > masked_from:
            keep = iota(part.shape, 0) + (at - masked_from) <= iota(part.shape, 1)
            part = jnp.where(keep, part, NEGATIVE)
        weights = jnp.exp2(part - log_total)
        if probs is not None:
            probs[rows, :] = weights.astype(BF16)
        mixed[rows, :] = (weights * (products[rows] - center)).astype(BF16)


def own_gradients_kernel(
    heads, pos, own, key, value, totals, key_out, value_out, *rest
):
    *pieces, terms, mixed, probs = rest
    helper = pos[1]
    rows = own.shape[1] - INFO
    length = key.shape[0]
    helpers = length // rows
    for head in range(heads):
        hc = cols_of(head)
        turned = key[:, hc].T
        for start in reversed(range(0, length, TILE)):
            end = start + TILE
            q = own_tile(own, helper, start, rows, head_cols(head, heads, 0))
            g = own_tile(own, helper, start, rows, head_cols(head, heads, 1))
            log_total = totals[2 * head : 2 * head + 1, start:end]
            center = totals[2 * head + 1 : 2 * head + 2, start:end]
            mixed_into(
                mixed, probs, key[0:end, hc], value[0:end, hc], q, g, log_total, center, start
            )
            value_new = dot(probs[0:end, :], g, 1, 0)
            key_new = dot(mixed[0:end, :], q, 1, 0)
            if end == length:
                value_out[:, hc] = value_new
                key_out[:, hc] = key_new
            else:
                value_out[0:end, hc] += value_new
                key_out[0:end, hc] += key_new
            query_new = (dot(turned[:, 0:end], mixed[0:end, :], 1, 0) * SCALING).T
            terms[start:end, hc] = query_new
    for k in range(helpers):
        at = pl.ds(pl.multiple_of((helper ^ k) * rows, rows), rows)
        piece_ref(pieces, k)[...] = terms[at, :].astype(BF16)


def slot_row(slots, tile, head, which, group):
    cut = slice(which * group, (which + 1) * group)
    count = TILE // group
    return jnp.concatenate(
        [slots[tile * count + a, head : head + 1, cut] for a in range(count)], axis=1
    )


def routed_query_kernel(heads, routed, key, value, slots, out, mixed):
    helpers, blocks, capacity, _ = routed.shape
    group = helpers * capacity
    count = TILE // group
    length = key.shape[0]

    def body(tile, _):
        rows = [
            slot_row(slots, tile, head, which, group) for head in range(heads) for which in range(2)
        ]
        pad = jnp.zeros((8 - len(rows), TILE), F32)
        columns = jnp.concatenate(rows + [pad], axis=0).T
        for head in range(heads):
            hc = cols_of(head)
            q = routed_tile(routed, tile, head_cols(head, heads, 0))
            g = routed_tile(routed, tile, head_cols(head, heads, 1))
            log_total = columns[:, 2 * head : 2 * head + 1]
            center = columns[:, 2 * head + 1 : 2 * head + 2]
            for at in range(0, length, STRIP):
                keys = slice(at, at + STRIP)
                scores = dot(q, key[keys, hc], 1, 1) * (SCALING * LOG2E)
                products = dot(g, value[keys, hc], 1, 1)
                weights = jnp.exp2(scores - log_total)
                mixed[head, :, keys] = (weights * (products - center)).astype(BF16)
            query_new = dot(mixed[head], key[:, hc], 1, 0) * SCALING
            for a in range(count):
                out[:, tile * count + a, :, hc] = (
                    query_new[a * group : (a + 1) * group]
                    .reshape(helpers, capacity, HEAD_DIM)
                    .astype(BF16)
                )
        return 0

    lax.fori_loop(0, blocks // count, body, 0)


def routed_block_kernel(
    heads, helpers, pos, routed, key, value, slots, key_own, value_own, *rest
):
    *pieces, key_acc, value_acc, mixed, probs = rest
    _, blocks, capacity, _ = routed.shape
    group = helpers * capacity
    key_acc[...] = key_own[...]
    value_acc[...] = value_own[...]

    def body(tile, _):
        for head in range(heads):
            hc = cols_of(head)
            q = routed_tile(routed, tile, head_cols(head, heads, 0))
            g = routed_tile(routed, tile, head_cols(head, heads, 1))
            log_total = slot_row(slots, tile, head, 0, group)
            center = slot_row(slots, tile, head, 1, group)
            mixed_into(
                mixed.at[head],
                probs.at[head],
                key[:, hc],
                value[:, hc],
                q,
                g,
                log_total,
                center,
                None,
            )
            value_acc[:, hc] += dot(probs[head], g, 1, 0)
            key_acc[:, hc] += dot(mixed[head], q, 1, 0)
        return 0

    lax.fori_loop(0, blocks * group // TILE, body, 0)
    width = key_acc.shape[1]
    share = key_acc.shape[0] // helpers
    for k in range(helpers):
        at = pl.ds(pl.multiple_of((pos[1] ^ k) * share, share), share)
        piece = piece_ref(pieces, k)
        piece[:, 0:width] = (key_acc[at, :] * SCALING).astype(BF16)
        piece[:, width : 2 * width] = value_acc[at, :].astype(BF16)


def place_kernel(helpers, pos, *refs):
    pieces = refs[:helpers]
    key_out, value_out = refs[helpers:]
    width = key_out.shape[1] // helpers
    for k in range(helpers):
        cols = pl.ds(pl.multiple_of((pos[1] ^ k) * width, width), width)
        key_out[:, cols] = pieces[k][:, 0:width]
        value_out[:, cols] = pieces[k][:, width : 2 * width]


def finish_kernel(helpers, pos, picker, returned, *refs):
    pieces = refs[:helpers]
    out = refs[helpers]
    width = out.shape[1] // helpers
    slots = picker.shape[1]
    for k in range(helpers):
        d = pos[1] ^ k
        cols = pl.ds(pl.multiple_of(d * width, width), width)
        terms = returned[d].astype(F32).reshape(slots, width).astype(BF16)
        out[:, cols] = (dot(picker[...], terms, 1, 0) + pieces[k][...].astype(F32)).astype(
            BF16
        )


DIRECT = (1, 3, 6)
RELAYED = ((2, 4, 6), (7, 5, 2))


def piece_shapes(shape, dtype, kind=pltpu.VMEM):
    one = kind(shape, dtype)
    pair = kind((2,) + shape, dtype)
    return [one] * (1 + len(DIRECT)) + [pair] * len(RELAYED)


def piece_ref(refs, k):
    if k == 0:
        return refs[0]
    if k in DIRECT:
        return refs[1 + DIRECT.index(k)]
    for n, (near, far, _) in enumerate(RELAYED):
        if k in (near, far):
            return refs[1 + len(DIRECT) + n].at[(near, far).index(k)]
    raise ValueError(k)


def exchange(pieces, helpers):
    def send(array, k):
        return lax.ppermute(array, "help", [(i, i ^ k) for i in range(helpers)])

    received = {0: pieces[0]}
    pairs = []
    for n, (near, _, _) in enumerate(RELAYED):
        pairs.append(send(pieces[1 + len(DIRECT) + n], near))
    for n, k in enumerate(DIRECT):
        received[k] = send(pieces[1 + n], k)
    for pair, (near, far, last) in zip(pairs, RELAYED):
        received[near] = pair[0]
        received[far] = send(pair[1], last)
    return [received[k] for k in range(helpers)]


def resident(x):
    return pltpu.with_memory_space_constraint(x, pltpu.VMEM)


def call(kernel, outputs, operands, position=None, scratch=(), flops=0, fast=99):
    vmem = pl.BlockSpec(memory_space=pltpu.VMEM)
    operands = [resident(x) if n < fast else x for n, x in enumerate(operands)]
    specs = [vmem] * len(operands)
    if position is not None:
        operands = [position] + list(operands)
        specs = [pl.BlockSpec(memory_space=pltpu.SMEM)] + specs
    return pl.pallas_call(
        kernel,
        out_shape=outputs,
        in_specs=specs,
        scratch_shapes=scratch,
        compiler_params=pltpu.CompilerParams(vmem_limit_bytes=VMEM_BYTES),
        cost_estimate=pl.CostEstimate(flops=flops, bytes_accessed=0, transcendentals=0),
    )(*operands)


def swap(array, axes):
    return lax.all_to_all(array, axes, split_axis=0, concat_axis=0, tiled=True)


def per_device(query_rows, key_rows, value_rows, output_grad, block_choice):
    blocks = lax.axis_size("ctx")
    helpers = lax.axis_size("help")
    helper = lax.axis_index("help")
    position = jnp.stack([lax.axis_index("ctx"), helper]).astype(jnp.int32)
    _, rows, features = query_rows.shape
    length = key_rows.shape[1]
    width = features // helpers
    heads = width // HEAD_DIM
    group = helpers * CAPACITY
    slots = blocks * CAPACITY
    share = length // helpers
    pairs = 2 * blocks * group * length * width
    shape = jax.ShapeDtypeStruct
    fast = pltpu.VMEM
    everyone = ("help", "ctx")

    sent, picker, *pieces = call(
        functools.partial(pack_kernel, blocks, helpers),
        [fast((helpers, blocks, CAPACITY, 2 * width), BF16), shape((rows, slots), BF16)]
        + piece_shapes((rows + INFO, 2 * width), BF16),
        [jnp.transpose(block_choice[0]), query_rows[0], output_grad[0]],
        position,
        flops=2 * rows * slots * features * 2,
        fast=0,
    )
    own = jnp.stack(exchange(pieces, helpers))
    routed = swap(sent.reshape(blocks * helpers, CAPACITY, 2 * width), everyone)
    routed = routed.reshape(helpers, blocks, CAPACITY, 2 * width)

    key = lax.dynamic_slice_in_dim(key_rows[0], helper * width, width, 1)
    value = lax.dynamic_slice_in_dim(value_rows[0], helper * width, width, 1)
    stats = call(
        functools.partial(own_statistics_kernel, heads, helpers),
        fast((2 * heads + 4, length), F32),
        [own, key, value],
        position,
        flops=pairs // 2,
    )
    slot_shape = fast((blocks, heads, 2 * group), F32)
    parts = call(
        functools.partial(routed_statistics_kernel, heads),
        slot_shape,
        [routed, key, value],
        flops=2 * pairs,
    )
    parts = swap(parts, "ctx")

    totals, spread = call(
        functools.partial(combine_kernel, heads, helpers),
        [fast((2 * heads, length), F32), slot_shape],
        [stats, parts],
        flops=pairs // 8,
    )
    spread = swap(spread, "ctx")

    tile = (heads, length, TILE)
    own_out = call(
        functools.partial(own_gradients_kernel, heads),
        [shape((length, width), F32)] * 2 + piece_shapes((rows, width), BF16, shape),
        [own, key, value, totals],
        position,
        [pltpu.VMEM((length, width), F32)] + [pltpu.VMEM(tile[1:], BF16)] * 2,
        flops=2 * pairs,
    )
    key_own, value_own, *query_own = own_out
    spread, key_own, value_own = lax.optimization_barrier((spread, key_own, value_own))
    query_own = exchange(query_own, helpers)

    terms = call(
        functools.partial(routed_query_kernel, heads),
        fast((helpers, blocks, CAPACITY, width), BF16),
        [routed, key, value, spread],
        scratch=[pltpu.VMEM((heads, TILE, length), BF16)],
        flops=3 * pairs,
    )
    returned = swap(terms.reshape(blocks * helpers, CAPACITY, width), everyone)
    returned = returned.reshape(helpers, blocks, CAPACITY, width)

    pieces = call(
        functools.partial(routed_block_kernel, heads, helpers),
        piece_shapes((share, 2 * width), BF16),
        [routed, key, value, spread, key_own, value_own],
        position,
        [pltpu.VMEM((length, width), F32)] * 2 + [pltpu.VMEM(tile, BF16)] * 2,
        flops=4 * pairs,
        fast=4,
    )
    pieces = exchange(pieces, helpers)

    key_grad, value_grad = call(
        functools.partial(place_kernel, helpers),
        [shape((share, features), BF16)] * 2,
        pieces,
        position,
    )
    query_grad = call(
        functools.partial(finish_kernel, helpers),
        shape((rows, features), BF16),
        [picker, returned, *query_own],
        position,
    )
    return query_grad[None], key_grad[None], value_grad[None]


def solution(mesh):
    split = P(None, ("ctx", "help"), None)
    shared = P(None, "ctx", None)

    return jax.shard_map(
        per_device,
        mesh=mesh,
        in_specs=(split, shared, shared, split, split),
        out_specs=(split, split, split),
        check_vma=False,
    )
```

```python
import functools

import jax
import jax.numpy as jnp
from jax import lax
from jax.experimental import pallas as pl
from jax.experimental.pallas import tpu as pltpu
from jax.sharding import PartitionSpec as P


HEAD_DIM = 128
CAPACITY = 8
NEGATIVE = -1e30
LOG2E = 1.4426950408889634
SCALING = HEAD_DIM ** (-0.5)
INFO = 16
TILE = 256
CHUNK = 64
VMEM_BYTES = 24 * 2**20
F32 = jnp.float32
BF16 = jnp.bfloat16


def iota(shape, dim):
    return lax.broadcasted_iota(jnp.int32, shape, dim)


def dot(a, b, ca, cb, precision=None):
    return lax.dot_general(
        a, b, (((ca,), (cb,)), ((), ())), precision=precision, preferred_element_type=F32
    )


def pack_kernel(blocks, helpers, pos, choice, query, grad, sent, picker_out, *own):
    rows = query.shape[0]
    width = query.shape[1] // helpers
    center = pos[0]
    helper = pos[1]
    slots = blocks * CAPACITY
    targets = []
    matches = []
    block_ids = iota((blocks, rows), 0)
    for r in range(2):
        c = choice[r : r + 1, :]
        t = jnp.where(c < center, center - 1 - c, -1)
        targets.append(t)
        matches.append(block_ids == t)
    counts = jnp.where(matches[0], 1.0, 0.0) + jnp.where(matches[1], 1.0, 0.0)
    before = jnp.where(iota((rows, rows), 0) < iota((rows, rows), 1), 1.0, 0.0).astype(BF16)
    earlier = dot(counts.astype(BF16), before, 1, 0)
    picker = jnp.zeros((slots, rows), F32)
    places = []
    for r in range(2):
        p = jnp.sum(jnp.where(matches[r], earlier, 0.0), axis=0, keepdims=True)
        places.append(p)
        code = jnp.where(targets[r] >= 0, targets[r] * CAPACITY + p.astype(jnp.int32), -1)
        picker = picker + jnp.where(iota((slots, rows), 0) == code, 1.0, 0.0)
    picker_out[...] = picker.T.astype(BF16)
    low = picker.astype(BF16)
    for d in range(helpers):
        for n, source in enumerate((query, grad)):
            got = dot(low, source[:, d * width : (d + 1) * width], 1, 0)
            sent[d, :, :, n * width : (n + 1) * width] = got.reshape(
                blocks, CAPACITY, width
            ).astype(BF16)
    info = jnp.concatenate([t.astype(F32) for t in targets] + places, axis=1)
    info = jnp.broadcast_to(info, (INFO, info.shape[1])).astype(BF16)
    for k in range(helpers):
        cols = pl.ds(pl.multiple_of((helper ^ k) * width, width), width)
        piece = piece_ref(own, k)
        piece[0:rows, 0:width] = query[:, cols]
        piece[0:rows, width : 2 * width] = grad[:, cols]
        piece[rows : rows + INFO, :] = info


def head_cols(head, heads, which):
    at = (which * heads + head) * HEAD_DIM
    return slice(at, at + HEAD_DIM)


def cols_of(head):
    return slice(head * HEAD_DIM, (head + 1) * HEAD_DIM)


def own_tile(own, helper, start, rows, cols):
    parts = [own[helper ^ g, 0:rows, cols] for g in range(start // rows, (start + TILE) // rows)]
    return jnp.concatenate(parts, axis=0)


def routed_tile(routed, tile, cols):
    helpers, _, capacity, _ = routed.shape
    group = helpers * capacity
    count = TILE // group
    parts = [
        routed[:, tile * count + a, :, cols].astype(F32).reshape(group, HEAD_DIM)
        for a in range(count)
    ]
    return jnp.concatenate(parts, axis=0).astype(BF16)


def statistics_of(key, value, q, g, masked_from):
    scores = dot(key, q, 1, 1)
    products = dot(value, g, 1, 1)
    shape = (8, q.shape[0])
    highest = jnp.full(shape, NEGATIVE, F32)
    total = jnp.zeros(shape, F32)
    crossed = jnp.zeros(shape, F32)
    for at in range(0, key.shape[0], CHUNK):
        part = scores[at : at + CHUNK] * (SCALING * LOG2E)
        if masked_from is not None and at + CHUNK > masked_from:
            keep = iota(part.shape, 0) + (at - masked_from) <= iota(part.shape, 1)
            part = jnp.where(keep, part, NEGATIVE)
        part = part.reshape((CHUNK // 8,) + shape)
        newer = jnp.maximum(highest, jnp.max(part, axis=0))
        weights = jnp.exp2(part - newer)
        if masked_from is not None and at + CHUNK > masked_from:
            weights = jnp.where(keep.reshape(weights.shape), weights, 0.0)
        shrink = jnp.exp2(highest - newer)
        total = total * shrink + jnp.sum(weights, axis=0)
        crossed = crossed * shrink + jnp.sum(
            weights * products[at : at + CHUNK].reshape(part.shape), axis=0
        )
        highest = newer
    top = jnp.max(highest, axis=0, keepdims=True)
    shrink = jnp.exp2(highest - top)
    total = jnp.sum(total * shrink, axis=0, keepdims=True)
    crossed = jnp.sum(crossed * shrink, axis=0, keepdims=True)
    return top + jnp.log(total) * LOG2E, crossed / total


def own_statistics_kernel(heads, helpers, pos, own, key, value, out):
    helper = pos[1]
    rows = own.shape[1] - INFO
    length = key.shape[0]
    for head in range(heads):
        hc = cols_of(head)
        for start in range(0, length, TILE):
            end = start + TILE
            q = own_tile(own, helper, start, rows, head_cols(head, heads, 0))
            g = own_tile(own, helper, start, rows, head_cols(head, heads, 1))
            log_sum, mean = statistics_of(key[0:end, hc], value[0:end, hc], q, g, start)
            out[2 * head : 2 * head + 1, start:end] = log_sum
            out[2 * head + 1 : 2 * head + 2, start:end] = mean
    for n in range(4):
        parts = [
            own[helper ^ g, rows : rows + INFO, n * rows : (n + 1) * rows].astype(F32)[0:1]
            for g in range(helpers)
        ]
        out[2 * heads + n : 2 * heads + n + 1, :] = jnp.concatenate(parts, axis=1)


def routed_statistics_kernel(heads, routed, key, value, out):
    helpers, blocks, capacity, _ = routed.shape
    group = helpers * capacity
    count = TILE // group

    def body(tile, _):
        for head in range(heads):
            hc = cols_of(head)
            q = routed_tile(routed, tile, head_cols(head, heads, 0))
            g = routed_tile(routed, tile, head_cols(head, heads, 1))
            log_sum, mean = statistics_of(key[:, hc], value[:, hc], q, g, None)
            for a in range(count):
                cut = slice(a * group, (a + 1) * group)
                out[tile * count + a, head : head + 1, 0:group] = log_sum[:, cut]
                out[tile * count + a, head : head + 1, group : 2 * group] = mean[:, cut]
        return 0

    lax.fori_loop(0, blocks // count, body, 0)


def thirds(x, axis):
    high = x.astype(BF16)
    rest = x - high.astype(F32)
    middle = rest.astype(BF16)
    low = (rest - middle.astype(F32)).astype(BF16)
    return jnp.concatenate([high, middle, low], axis=axis)


def combine_kernel(heads, helpers, stats, got, totals, slots):
    length = stats.shape[1]
    blocks = got.shape[0]
    group = got.shape[2] // 2
    rows = length // helpers
    wide = 2 * group
    slot = iota((group, length), 0)
    in_group = (slot // CAPACITY) == (iota((group, length), 1) // rows)
    slot_place = (slot % CAPACITY).astype(F32)
    block_ids = iota((blocks, length), 0).astype(F32)
    hots = []
    masks = []
    present = []
    for r in range(2):
        t = stats[2 * heads + r : 2 * heads + r + 1, :]
        p = stats[2 * heads + 2 + r : 2 * heads + 3 + r, :]
        present.append(t >= 0.0)
        hots.append(jnp.where(block_ids == t, 1.0, 0.0).astype(BF16))
        masks.append(in_group & (slot_place == p) & (t >= 0.0))
    for head in range(heads):
        part = thirds(got[:, head, :].T, 1)
        logs = [stats[2 * head : 2 * head + 1, :]]
        means = [stats[2 * head + 1 : 2 * head + 2, :]]
        for r in range(2):
            hot = jnp.concatenate([hots[r]] * 3, axis=0)
            spread = dot(part, hot, 1, 0)
            log_r = jnp.sum(jnp.where(masks[r], spread[0:group], 0.0), axis=0, keepdims=True)
            mean_r = jnp.sum(jnp.where(masks[r], spread[group:wide], 0.0), axis=0, keepdims=True)
            logs.append(jnp.where(present[r], log_r, NEGATIVE))
            means.append(mean_r)
        top = jnp.maximum(jnp.maximum(logs[0], logs[1]), logs[2])
        shares = [jnp.exp2(v - top) for v in logs]
        norm = shares[0] + shares[1] + shares[2]
        log_total = top + jnp.log(norm) * LOG2E
        center = (shares[0] * means[0] + shares[1] * means[1] + shares[2] * means[2]) / norm
        totals[2 * head : 2 * head + 1, :] = log_total
        totals[2 * head + 1 : 2 * head + 2, :] = center
        logs3 = thirds(log_total, 0).astype(F32)
        means3 = thirds(center, 0).astype(F32)
        result = jnp.zeros((blocks, wide), F32)
        for r in range(2):
            for n in range(3):
                both = jnp.concatenate(
                    [
                        jnp.where(masks[r], logs3[n : n + 1], 0.0),
                        jnp.where(masks[r], means3[n : n + 1], 0.0),
                    ],
                    axis=0,
                ).astype(BF16)
                result = result + dot(hots[r], both, 1, 1)
        slots[:, head, :] = result


def mixed_into(mixed, probs, key, value, q, g, log_total, center, masked_from):
    scores = dot(key, q, 1, 1)
    products = dot(value, g, 1, 1)
    for at in range(0, key.shape[0], CHUNK):
        rows = slice(at, at + CHUNK)
        part = scores[rows] * (SCALING * LOG2E)
        if masked_from is not None and at + CHUNK > masked_from:
            keep = iota(part.shape, 0) + (at - masked_from) <= iota(part.shape, 1)
            part = jnp.where(keep, part, NEGATIVE)
        weights = jnp.exp2(part - log_total)
        if probs is not None:
            probs[rows, :] = weights.astype(BF16)
        mixed[rows, :] = (weights * (products[rows] - center)).astype(BF16)


def own_gradients_kernel(heads, pos, own, key, value, totals, key_out, value_out, *rest):
    *pieces, terms, mixed, probs = rest
    helper = pos[1]
    rows = own.shape[1] - INFO
    length = key.shape[0]
    for head in range(heads):
        hc = cols_of(head)
        turned = key[:, hc].T
        for start in reversed(range(0, length, TILE)):
            end = start + TILE
            q = own_tile(own, helper, start, rows, head_cols(head, heads, 0))
            g = own_tile(own, helper, start, rows, head_cols(head, heads, 1))
            log_total = totals[2 * head : 2 * head + 1, start:end]
            center = totals[2 * head + 1 : 2 * head + 2, start:end]
            mixed_into(
                mixed, probs, key[0:end, hc], value[0:end, hc], q, g, log_total, center, start
            )
            value_new = dot(g.T, probs[0:end, :], 1, 1)
            key_new = dot(q.T, mixed[0:end, :], 1, 1)
            if end == length:
                value_out[hc, :] = value_new
                key_out[hc, :] = key_new
            else:
                value_out[hc, 0:end] += value_new
                key_out[hc, 0:end] += key_new
            terms[start:end, hc] = (dot(turned[:, 0:end], mixed[0:end, :], 1, 0) * SCALING).T
    for k in range(length // rows):
        at = pl.ds(pl.multiple_of((helper ^ k) * rows, rows), rows)
        piece_ref(pieces, k)[...] = terms[at, :].astype(BF16)


def slot_row(slots, tile, head, which, group):
    cut = slice(which * group, (which + 1) * group)
    count = TILE // group
    return jnp.concatenate(
        [slots[tile * count + a, head : head + 1, cut] for a in range(count)], axis=1
    )


def routed_gradients_kernel(
    heads, helpers, pos, routed, key, value, slots, key_own, value_own, out, *rest
):
    *pieces, key_acc, value_acc, mixed, probs = rest
    _, blocks, capacity, _ = routed.shape
    group = helpers * capacity
    count = TILE // group
    key_acc[...] = key_own[...]
    value_acc[...] = value_own[...]
    turned = [key[:, cols_of(head)].T for head in range(heads)]

    def body(tile, _):
        for head in range(heads):
            hc = cols_of(head)
            q = routed_tile(routed, tile, head_cols(head, heads, 0))
            g = routed_tile(routed, tile, head_cols(head, heads, 1))
            log_total = slot_row(slots, tile, head, 0, group)
            center = slot_row(slots, tile, head, 1, group)
            low = mixed.at[head]
            high = probs.at[head]
            mixed_into(low, high, key[:, hc], value[:, hc], q, g, log_total, center, None)
            value_acc[hc, :] += dot(g.T, high[...], 1, 1)
            key_acc[hc, :] += dot(q.T, low[...], 1, 1)
            query_new = (dot(turned[head], low[...], 1, 0) * SCALING).T
            for a in range(count):
                out[:, tile * count + a, :, hc] = (
                    query_new[a * group : (a + 1) * group]
                    .reshape(helpers, capacity, HEAD_DIM)
                    .astype(BF16)
                )
        return 0

    lax.fori_loop(0, blocks // count, body, 0)
    width = key_acc.shape[0]
    share = key_acc.shape[1] // helpers
    for k in range(helpers):
        at = pl.ds(pl.multiple_of((pos[1] ^ k) * share, share), share)
        piece = piece_ref(pieces, k)
        piece[:, 0:width] = (key_acc[:, at] * SCALING).T.astype(BF16)
        piece[:, width : 2 * width] = value_acc[:, at].T.astype(BF16)


def place_kernel(helpers, pos, *refs):
    pieces = refs[:helpers]
    key_out, value_out = refs[helpers:]
    width = key_out.shape[1] // helpers
    for k in range(helpers):
        cols = pl.ds(pl.multiple_of((pos[1] ^ k) * width, width), width)
        key_out[:, cols] = pieces[k][:, 0:width]
        value_out[:, cols] = pieces[k][:, width : 2 * width]


def finish_kernel(helpers, pos, picker, returned, *refs):
    pieces = refs[:helpers]
    out = refs[helpers]
    width = out.shape[1] // helpers
    slots = picker.shape[1]
    for k in range(helpers):
        d = pos[1] ^ k
        cols = pl.ds(pl.multiple_of(d * width, width), width)
        terms = returned[d].astype(F32).reshape(slots, width).astype(BF16)
        out[:, cols] = (dot(picker[...], terms, 1, 0) + pieces[k][...].astype(F32)).astype(
            BF16
        )


DIRECT = (1, 3, 6)
RELAYED = ((2, 4, 6), (7, 5, 2))


def piece_shapes(shape, dtype, kind=pltpu.VMEM):
    one = kind(shape, dtype)
    pair = kind((2,) + shape, dtype)
    return [one] * (1 + len(DIRECT)) + [pair] * len(RELAYED)


def piece_ref(refs, k):
    if k == 0:
        return refs[0]
    if k in DIRECT:
        return refs[1 + DIRECT.index(k)]
    for n, (near, far, _) in enumerate(RELAYED):
        if k in (near, far):
            return refs[1 + len(DIRECT) + n].at[(near, far).index(k)]
    raise ValueError(k)


def exchange(pieces, helpers):
    def send(array, k):
        return lax.ppermute(array, "help", [(i, i ^ k) for i in range(helpers)])

    received = {0: pieces[0]}
    pairs = []
    for n, (near, _, _) in enumerate(RELAYED):
        pairs.append(send(pieces[1 + len(DIRECT) + n], near))
    for n, k in enumerate(DIRECT):
        received[k] = send(pieces[1 + n], k)
    for pair, (near, far, last) in zip(pairs, RELAYED):
        received[near] = pair[0]
        received[far] = send(pair[1], last)
    return [received[k] for k in range(helpers)]


def call(kernel, outputs, operands, position=None, scratch=(), flops=0, fast=99):
    vmem = pl.BlockSpec(memory_space=pltpu.VMEM)
    operands = [
        pltpu.with_memory_space_constraint(x, pltpu.VMEM if n < fast else pltpu.HBM)
        for n, x in enumerate(operands)
    ]
    specs = [vmem] * len(operands)
    if position is not None:
        operands = [position] + list(operands)
        specs = [pl.BlockSpec(memory_space=pltpu.SMEM)] + specs
    return pl.pallas_call(
        kernel,
        out_shape=outputs,
        in_specs=specs,
        scratch_shapes=scratch,
        compiler_params=pltpu.CompilerParams(vmem_limit_bytes=VMEM_BYTES),
        cost_estimate=pl.CostEstimate(flops=flops, bytes_accessed=0, transcendentals=0),
    )(*operands)


def swap(array, axes):
    return lax.all_to_all(array, axes, split_axis=0, concat_axis=0, tiled=True)


def per_device(query_rows, key_rows, value_rows, output_grad, block_choice):
    blocks = lax.axis_size("ctx")
    helpers = lax.axis_size("help")
    helper = lax.axis_index("help")
    position = jnp.stack([lax.axis_index("ctx"), helper]).astype(jnp.int32)
    _, rows, features = query_rows.shape
    length = key_rows.shape[1]
    width = features // helpers
    heads = width // HEAD_DIM
    group = helpers * CAPACITY
    slots = blocks * CAPACITY
    share = length // helpers
    pairs = 2 * blocks * group * length * width
    shape = jax.ShapeDtypeStruct
    fast = pltpu.VMEM
    everyone = ("help", "ctx")

    sent, picker, *pieces = call(
        functools.partial(pack_kernel, blocks, helpers),
        [pltpu.HBM((helpers, blocks, CAPACITY, 2 * width), BF16), shape((rows, slots), BF16)]
        + piece_shapes((rows + INFO, 2 * width), BF16),
        [jnp.transpose(block_choice[0]), query_rows[0], output_grad[0]],
        position,
        flops=2 * rows * slots * features * 2,
        fast=0,
    )
    own = jnp.stack(exchange(pieces, helpers))
    routed = swap(sent.reshape(blocks * helpers, CAPACITY, 2 * width), everyone)
    routed = routed.reshape(helpers, blocks, CAPACITY, 2 * width)

    key = lax.dynamic_slice_in_dim(key_rows[0], helper * width, width, 1)
    value = lax.dynamic_slice_in_dim(value_rows[0], helper * width, width, 1)
    stats = call(
        functools.partial(own_statistics_kernel, heads, helpers),
        fast((2 * heads + 4, length), F32),
        [own, key, value],
        position,
        flops=pairs // 2,
    )
    slot_shape = fast((blocks, heads, 2 * group), F32)
    parts = call(
        functools.partial(routed_statistics_kernel, heads),
        slot_shape,
        [routed, key, value],
        flops=2 * pairs,
    )
    parts = swap(parts, "ctx")

    totals, spread = call(
        functools.partial(combine_kernel, heads, helpers),
        [fast((2 * heads, length), F32), slot_shape],
        [stats, parts],
        flops=pairs // 8,
    )
    spread = swap(spread, "ctx")

    tile = (heads, length, TILE)
    own_out = call(
        functools.partial(own_gradients_kernel, heads),
        [pltpu.HBM((width, length), F32)] * 2 + piece_shapes((rows, width), BF16, pltpu.HBM),
        [own, key, value, totals],
        position,
        [pltpu.VMEM((length, width), F32)] + [pltpu.VMEM(tile[1:], BF16)] * 2,
        flops=2 * pairs,
    )
    key_own, value_own, *query_own = own_out
    spread, key_own, value_own = lax.optimization_barrier((spread, key_own, value_own))
    query_own = exchange(query_own, helpers)

    terms, *pieces = call(
        functools.partial(routed_gradients_kernel, heads, helpers),
        [pltpu.HBM((helpers, blocks, CAPACITY, width), BF16)] + piece_shapes((share, 2 * width), BF16, pltpu.HBM),
        [routed, key, value, spread, key_own, value_own],
        position,
        [pltpu.VMEM((width, length), F32)] * 2 + [pltpu.VMEM(tile, BF16)] * 2,
        flops=5 * pairs,
        fast=4,
    )
    returned = swap(terms.reshape(blocks * helpers, CAPACITY, width), everyone)
    returned = returned.reshape(helpers, blocks, CAPACITY, width)

    pieces = exchange(pieces, helpers)

    key_grad, value_grad = call(
        functools.partial(place_kernel, helpers),
        [shape((share, features), BF16)] * 2,
        pieces,
        position,
    )
    query_grad = call(
        functools.partial(finish_kernel, helpers),
        shape((rows, features), BF16),
        [picker, returned, *query_own],
        position,
    )
    return query_grad[None], key_grad[None], value_grad[None]


def solution(mesh):
    split = P(None, ("ctx", "help"), None)
    shared = P(None, "ctx", None)

    return jax.shard_map(
        per_device,
        mesh=mesh,
        in_specs=(split, shared, shared, split, split),
        out_specs=(split, split, split),
        check_vma=False,
    )
```

```python
import functools

import jax
import jax.numpy as jnp
from jax import lax
from jax.experimental import pallas as pl
from jax.experimental.pallas import tpu as pltpu
from jax.sharding import PartitionSpec as P


HEAD_DIM = 128
CAPACITY = 8
NEGATIVE = -1e30
LOG2E = 1.4426950408889634
SCALING = HEAD_DIM ** (-0.5)
INFO = 16
TILE = 256
WIDE_TILE = 512
CHUNK = 64
VMEM_BYTES = 24 * 2**20
F32 = jnp.float32
BF16 = jnp.bfloat16


def iota(shape, dim):
    return lax.broadcasted_iota(jnp.int32, shape, dim)


def dot(a, b, ca, cb, precision=None):
    return lax.dot_general(
        a, b, (((ca,), (cb,)), ((), ())), precision=precision, preferred_element_type=F32
    )


def pack_kernel(blocks, helpers, pos, choice, query, grad, sent, picker_out, *own):
    rows = query.shape[0]
    width = query.shape[1] // helpers
    center = pos[0]
    helper = pos[1]
    slots = blocks * CAPACITY
    targets = []
    matches = []
    block_ids = iota((blocks, rows), 0)
    for r in range(2):
        c = choice[r : r + 1, :]
        t = jnp.where(c < center, center - 1 - c, -1)
        targets.append(t)
        matches.append(block_ids == t)
    counts = jnp.where(matches[0], 1.0, 0.0) + jnp.where(matches[1], 1.0, 0.0)
    before = jnp.where(iota((rows, rows), 0) < iota((rows, rows), 1), 1.0, 0.0).astype(BF16)
    earlier = dot(counts.astype(BF16), before, 1, 0)
    picker = jnp.zeros((slots, rows), F32)
    places = []
    for r in range(2):
        p = jnp.sum(jnp.where(matches[r], earlier, 0.0), axis=0, keepdims=True)
        places.append(p)
        code = jnp.where(targets[r] >= 0, targets[r] * CAPACITY + p.astype(jnp.int32), -1)
        picker = picker + jnp.where(iota((slots, rows), 0) == code, 1.0, 0.0)
    picker_out[...] = picker.T.astype(BF16)
    low = picker.astype(BF16)
    for d in range(helpers):
        for n, source in enumerate((query, grad)):
            got = dot(low, source[:, d * width : (d + 1) * width], 1, 0)
            sent[d, :, :, n * width : (n + 1) * width] = got.reshape(
                blocks, CAPACITY, width
            ).astype(BF16)
    info = jnp.concatenate([t.astype(F32) for t in targets] + places, axis=1)
    info = jnp.broadcast_to(info, (INFO, info.shape[1])).astype(BF16)
    for k in range(helpers):
        cols = pl.ds(pl.multiple_of((helper ^ k) * width, width), width)
        piece = piece_ref(own, k)
        piece[0:rows, 0:width] = query[:, cols]
        piece[0:rows, width : 2 * width] = grad[:, cols]
        piece[rows : rows + INFO, :] = info


def head_cols(head, heads, which):
    at = (which * heads + head) * HEAD_DIM
    return slice(at, at + HEAD_DIM)


def cols_of(head):
    return slice(head * HEAD_DIM, (head + 1) * HEAD_DIM)


def own_tile(own, helper, start, rows, cols):
    parts = [own[helper ^ g, 0:rows, cols] for g in range(start // rows, (start + TILE) // rows)]
    return jnp.concatenate(parts, axis=0)


def routed_tile(routed, tile, count, cols):
    helpers, _, capacity, _ = routed.shape
    group = helpers * capacity
    parts = [
        routed[:, tile * count + a, :, cols].astype(F32).reshape(group, HEAD_DIM)
        for a in range(count)
    ]
    return jnp.concatenate(parts, axis=0).astype(BF16)


def statistics_of(key, value, q, g, masked_from):
    scores = dot(key, q, 1, 1)
    products = dot(value, g, 1, 1)
    shape = (8, q.shape[0])
    highest = jnp.full(shape, NEGATIVE, F32)
    total = jnp.zeros(shape, F32)
    crossed = jnp.zeros(shape, F32)
    for at in range(0, key.shape[0], CHUNK):
        part = scores[at : at + CHUNK] * (SCALING * LOG2E)
        if masked_from is not None and at + CHUNK > masked_from:
            keep = iota(part.shape, 0) + (at - masked_from) <= iota(part.shape, 1)
            part = jnp.where(keep, part, NEGATIVE)
        part = part.reshape((CHUNK // 8,) + shape)
        newer = jnp.maximum(highest, jnp.max(part, axis=0))
        weights = jnp.exp2(part - newer)
        if masked_from is not None and at + CHUNK > masked_from:
            weights = jnp.where(keep.reshape(weights.shape), weights, 0.0)
        shrink = jnp.exp2(highest - newer)
        total = total * shrink + jnp.sum(weights, axis=0)
        crossed = crossed * shrink + jnp.sum(
            weights * products[at : at + CHUNK].reshape(part.shape), axis=0
        )
        highest = newer
    top = jnp.max(highest, axis=0, keepdims=True)
    shrink = jnp.exp2(highest - top)
    total = jnp.sum(total * shrink, axis=0, keepdims=True)
    crossed = jnp.sum(crossed * shrink, axis=0, keepdims=True)
    return top + jnp.log(total) * LOG2E, crossed / total


def own_statistics_kernel(heads, helpers, pos, own, key, value, out):
    helper = pos[1]
    rows = own.shape[1] - INFO
    length = key.shape[0]
    for head in range(heads):
        hc = cols_of(head)
        for start in range(0, length, TILE):
            end = start + TILE
            q = own_tile(own, helper, start, rows, head_cols(head, heads, 0))
            g = own_tile(own, helper, start, rows, head_cols(head, heads, 1))
            log_sum, mean = statistics_of(key[0:end, hc], value[0:end, hc], q, g, start)
            out[2 * head : 2 * head + 1, start:end] = log_sum
            out[2 * head + 1 : 2 * head + 2, start:end] = mean
    for n in range(4):
        parts = [
            own[helper ^ g, rows : rows + INFO, n * rows : (n + 1) * rows].astype(F32)[0:1]
            for g in range(helpers)
        ]
        out[2 * heads + n : 2 * heads + n + 1, :] = jnp.concatenate(parts, axis=1)


def routed_statistics_kernel(heads, routed, key, value, out):
    helpers, blocks, capacity, _ = routed.shape
    group = helpers * capacity
    count = TILE // group

    def body(tile, _):
        for head in range(heads):
            hc = cols_of(head)
            q = routed_tile(routed, tile, count, head_cols(head, heads, 0))
            g = routed_tile(routed, tile, count, head_cols(head, heads, 1))
            log_sum, mean = statistics_of(key[:, hc], value[:, hc], q, g, None)
            for a in range(count):
                cut = slice(a * group, (a + 1) * group)
                out[tile * count + a, head : head + 1, 0:group] = log_sum[:, cut]
                out[tile * count + a, head : head + 1, group : 2 * group] = mean[:, cut]
        return 0

    lax.fori_loop(0, blocks // count, body, 0)


def thirds(x, axis):
    high = x.astype(BF16)
    rest = x - high.astype(F32)
    middle = rest.astype(BF16)
    low = (rest - middle.astype(F32)).astype(BF16)
    return jnp.concatenate([high, middle, low], axis=axis)


def combine_kernel(heads, helpers, stats, got, totals, slots):
    length = stats.shape[1]
    blocks = got.shape[0]
    group = got.shape[2] // 2
    rows = length // helpers
    wide = 2 * group
    slot = iota((group, length), 0)
    in_group = (slot // CAPACITY) == (iota((group, length), 1) // rows)
    slot_place = (slot % CAPACITY).astype(F32)
    block_ids = iota((blocks, length), 0).astype(F32)
    hots = []
    masks = []
    present = []
    for r in range(2):
        t = stats[2 * heads + r : 2 * heads + r + 1, :]
        p = stats[2 * heads + 2 + r : 2 * heads + 3 + r, :]
        present.append(t >= 0.0)
        hots.append(jnp.where(block_ids == t, 1.0, 0.0).astype(BF16))
        masks.append(in_group & (slot_place == p) & (t >= 0.0))
    for head in range(heads):
        part = thirds(got[:, head, :].T, 1)
        logs = [stats[2 * head : 2 * head + 1, :]]
        means = [stats[2 * head + 1 : 2 * head + 2, :]]
        for r in range(2):
            hot = jnp.concatenate([hots[r]] * 3, axis=0)
            spread = dot(part, hot, 1, 0)
            log_r = jnp.sum(jnp.where(masks[r], spread[0:group], 0.0), axis=0, keepdims=True)
            mean_r = jnp.sum(jnp.where(masks[r], spread[group:wide], 0.0), axis=0, keepdims=True)
            logs.append(jnp.where(present[r], log_r, NEGATIVE))
            means.append(mean_r)
        top = jnp.maximum(jnp.maximum(logs[0], logs[1]), logs[2])
        shares = [jnp.exp2(v - top) for v in logs]
        norm = shares[0] + shares[1] + shares[2]
        log_total = top + jnp.log(norm) * LOG2E
        center = (shares[0] * means[0] + shares[1] * means[1] + shares[2] * means[2]) / norm
        totals[2 * head : 2 * head + 1, :] = log_total
        totals[2 * head + 1 : 2 * head + 2, :] = center
        logs3 = thirds(log_total, 0).astype(F32)
        means3 = thirds(center, 0).astype(F32)
        result = jnp.zeros((blocks, wide), F32)
        for r in range(2):
            for n in range(3):
                both = jnp.concatenate(
                    [
                        jnp.where(masks[r], logs3[n : n + 1], 0.0),
                        jnp.where(masks[r], means3[n : n + 1], 0.0),
                    ],
                    axis=0,
                ).astype(BF16)
                result = result + dot(hots[r], both, 1, 1)
        slots[:, head, :] = result


def mixed_into(mixed, probs, key, value, q, g, log_total, center, masked_from):
    scores = dot(key, q, 1, 1)
    products = dot(value, g, 1, 1)
    for at in range(0, key.shape[0], CHUNK):
        rows = slice(at, at + CHUNK)
        part = scores[rows] * (SCALING * LOG2E)
        if masked_from is not None and at + CHUNK > masked_from:
            keep = iota(part.shape, 0) + (at - masked_from) <= iota(part.shape, 1)
            part = jnp.where(keep, part, NEGATIVE)
        weights = jnp.exp2(part - log_total)
        if probs is not None:
            probs[rows, :] = weights.astype(BF16)
        mixed[rows, :] = (weights * (products[rows] - center)).astype(BF16)


def own_gradients_kernel(heads, pos, own, key, value, totals, key_out, value_out, *rest):
    *pieces, terms, mixed, probs = rest
    helper = pos[1]
    rows = own.shape[1] - INFO
    length = key.shape[0]
    for head in range(heads):
        hc = cols_of(head)
        turned = key[:, hc].T
        for start in reversed(range(0, length, TILE)):
            end = start + TILE
            q = own_tile(own, helper, start, rows, head_cols(head, heads, 0))
            g = own_tile(own, helper, start, rows, head_cols(head, heads, 1))
            log_total = totals[2 * head : 2 * head + 1, start:end]
            center = totals[2 * head + 1 : 2 * head + 2, start:end]
            mixed_into(
                mixed, probs, key[0:end, hc], value[0:end, hc], q, g, log_total, center, start
            )
            value_new = dot(g.T, probs[0:end, :], 1, 1)
            key_new = dot(q.T, mixed[0:end, :], 1, 1)
            if end == length:
                value_out[hc, :] = value_new
                key_out[hc, :] = key_new
            else:
                value_out[hc, 0:end] += value_new
                key_out[hc, 0:end] += key_new
            terms[start:end, hc] = (dot(turned[:, 0:end], mixed[0:end, :], 1, 0) * SCALING).T
    for k in range(length // rows):
        at = pl.ds(pl.multiple_of((helper ^ k) * rows, rows), rows)
        piece_ref(pieces, k)[...] = terms[at, :].astype(BF16)


def slot_row(slots, tile, count, head, which, group):
    cut = slice(which * group, (which + 1) * group)
    return jnp.concatenate(
        [slots[tile * count + a, head : head + 1, cut] for a in range(count)], axis=1
    )


def routed_gradients_kernel(
    heads, helpers, pos, routed, key, value, slots, key_own, value_own, out, *rest
):
    *pieces, key_acc, value_acc, mixed, probs = rest
    _, blocks, capacity, _ = routed.shape
    group = helpers * capacity
    count = WIDE_TILE // group
    key_acc[...] = key_own[...]
    value_acc[...] = value_own[...]
    turned = [key[:, cols_of(head)].T for head in range(heads)]

    def body(tile, _):
        for head in range(heads):
            hc = cols_of(head)
            q = routed_tile(routed, tile, count, head_cols(head, heads, 0))
            g = routed_tile(routed, tile, count, head_cols(head, heads, 1))
            log_total = slot_row(slots, tile, count, head, 0, group)
            center = slot_row(slots, tile, count, head, 1, group)
            low = mixed.at[head]
            high = probs.at[head]
            mixed_into(low, high, key[:, hc], value[:, hc], q, g, log_total, center, None)
            value_acc[hc, :] += dot(g.T, high[...], 1, 1)
            key_acc[hc, :] += dot(q.T, low[...], 1, 1)
            query_new = (dot(turned[head], low[...], 1, 0) * SCALING).T
            for a in range(count):
                out[:, tile * count + a, :, hc] = (
                    query_new[a * group : (a + 1) * group]
                    .reshape(helpers, capacity, HEAD_DIM)
                    .astype(BF16)
                )
        return 0

    lax.fori_loop(0, blocks // count, body, 0)
    width = key_acc.shape[0]
    share = key_acc.shape[1] // helpers
    for k in range(helpers):
        at = pl.ds(pl.multiple_of((pos[1] ^ k) * share, share), share)
        piece = piece_ref(pieces, k)
        piece[:, 0:width] = (key_acc[:, at] * SCALING).T.astype(BF16)
        piece[:, width : 2 * width] = value_acc[:, at].T.astype(BF16)


def place_kernel(helpers, pos, *refs):
    pieces = refs[:helpers]
    key_out, value_out = refs[helpers:]
    width = key_out.shape[1] // helpers
    for k in range(helpers):
        cols = pl.ds(pl.multiple_of((pos[1] ^ k) * width, width), width)
        key_out[:, cols] = pieces[k][:, 0:width]
        value_out[:, cols] = pieces[k][:, width : 2 * width]


def finish_kernel(helpers, pos, picker, returned, *refs):
    pieces = refs[:helpers]
    out = refs[helpers]
    width = out.shape[1] // helpers
    slots = picker.shape[1]
    for k in range(helpers):
        d = pos[1] ^ k
        cols = pl.ds(pl.multiple_of(d * width, width), width)
        terms = returned[d].astype(F32).reshape(slots, width).astype(BF16)
        out[:, cols] = (dot(picker[...], terms, 1, 0) + pieces[k][...].astype(F32)).astype(
            BF16
        )


DIRECT = (1, 3, 6)
RELAYED = ((2, 4, 6), (7, 5, 2))


def piece_shapes(shape, dtype, kind=pltpu.VMEM):
    one = kind(shape, dtype)
    pair = kind((2,) + shape, dtype)
    return [one] * (1 + len(DIRECT)) + [pair] * len(RELAYED)


def piece_ref(refs, k):
    if k == 0:
        return refs[0]
    if k in DIRECT:
        return refs[1 + DIRECT.index(k)]
    for n, (near, far, _) in enumerate(RELAYED):
        if k in (near, far):
            return refs[1 + len(DIRECT) + n].at[(near, far).index(k)]
    raise ValueError(k)


def exchange(pieces, helpers):
    def send(array, k):
        return lax.ppermute(array, "help", [(i, i ^ k) for i in range(helpers)])

    received = {0: pieces[0]}
    pairs = []
    for n, (near, _, _) in enumerate(RELAYED):
        pairs.append(send(pieces[1 + len(DIRECT) + n], near))
    for n, k in enumerate(DIRECT):
        received[k] = send(pieces[1 + n], k)
    for pair, (near, far, last) in zip(pairs, RELAYED):
        received[near] = pair[0]
        received[far] = send(pair[1], last)
    return [received[k] for k in range(helpers)]


def call(kernel, outputs, operands, position=None, scratch=(), flops=0, fast=99):
    vmem = pl.BlockSpec(memory_space=pltpu.VMEM)
    operands = [
        pltpu.with_memory_space_constraint(x, pltpu.VMEM if n < fast else pltpu.HBM)
        for n, x in enumerate(operands)
    ]
    specs = [vmem] * len(operands)
    if position is not None:
        operands = [position] + list(operands)
        specs = [pl.BlockSpec(memory_space=pltpu.SMEM)] + specs
    return pl.pallas_call(
        kernel,
        out_shape=outputs,
        in_specs=specs,
        scratch_shapes=scratch,
        compiler_params=pltpu.CompilerParams(vmem_limit_bytes=VMEM_BYTES),
        cost_estimate=pl.CostEstimate(flops=flops, bytes_accessed=0, transcendentals=0),
    )(*operands)


def swap(array, axes):
    return lax.all_to_all(array, axes, split_axis=0, concat_axis=0, tiled=True)


def per_device(query_rows, key_rows, value_rows, output_grad, block_choice):
    blocks = lax.axis_size("ctx")
    helpers = lax.axis_size("help")
    helper = lax.axis_index("help")
    position = jnp.stack([lax.axis_index("ctx"), helper]).astype(jnp.int32)
    _, rows, features = query_rows.shape
    length = key_rows.shape[1]
    width = features // helpers
    heads = width // HEAD_DIM
    group = helpers * CAPACITY
    slots = blocks * CAPACITY
    share = length // helpers
    pairs = 2 * blocks * group * length * width
    shape = jax.ShapeDtypeStruct
    fast = pltpu.VMEM
    everyone = ("help", "ctx")

    sent, picker, *pieces = call(
        functools.partial(pack_kernel, blocks, helpers),
        [pltpu.HBM((helpers, blocks, CAPACITY, 2 * width), BF16), shape((rows, slots), BF16)]
        + piece_shapes((rows + INFO, 2 * width), BF16),
        [jnp.transpose(block_choice[0]), query_rows[0], output_grad[0]],
        position,
        flops=2 * rows * slots * features * 2,
        fast=0,
    )
    own = jnp.stack(exchange(pieces, helpers))
    routed = swap(sent.reshape(blocks * helpers, CAPACITY, 2 * width), everyone)
    routed = routed.reshape(helpers, blocks, CAPACITY, 2 * width)

    key = lax.dynamic_slice_in_dim(key_rows[0], helper * width, width, 1)
    value = lax.dynamic_slice_in_dim(value_rows[0], helper * width, width, 1)
    stats = call(
        functools.partial(own_statistics_kernel, heads, helpers),
        fast((2 * heads + 4, length), F32),
        [own, key, value],
        position,
        flops=pairs // 2,
    )
    slot_shape = fast((blocks, heads, 2 * group), F32)
    parts = call(
        functools.partial(routed_statistics_kernel, heads),
        slot_shape,
        [routed, key, value],
        flops=2 * pairs,
    )
    parts = swap(parts, "ctx")

    totals, spread = call(
        functools.partial(combine_kernel, heads, helpers),
        [fast((2 * heads, length), F32), slot_shape],
        [stats, parts],
        flops=pairs // 8,
    )
    spread = swap(spread, "ctx")

    own_out = call(
        functools.partial(own_gradients_kernel, heads),
        [pltpu.HBM((width, length), F32)] * 2 + piece_shapes((rows, width), BF16, pltpu.HBM),
        [own, key, value, totals],
        position,
        [pltpu.VMEM((length, width), F32)] + [pltpu.VMEM((length, TILE), BF16)] * 2,
        flops=2 * pairs,
    )
    key_own, value_own, *query_own = own_out
    spread, key_own, value_own = lax.optimization_barrier((spread, key_own, value_own))
    query_own = exchange(query_own, helpers)

    terms, *pieces = call(
        functools.partial(routed_gradients_kernel, heads, helpers),
        [pltpu.HBM((helpers, blocks, CAPACITY, width), BF16)] + piece_shapes((share, 2 * width), BF16, pltpu.HBM),
        [routed, key, value, spread, key_own, value_own],
        position,
        [pltpu.VMEM((width, length), F32)] * 2 + [pltpu.VMEM((heads, length, WIDE_TILE), BF16)] * 2,
        flops=5 * pairs,
        fast=4,
    )
    returned = swap(terms.reshape(blocks * helpers, CAPACITY, width), everyone)
    returned = returned.reshape(helpers, blocks, CAPACITY, width)

    pieces = exchange(pieces, helpers)

    query_grad = call(
        functools.partial(finish_kernel, helpers),
        shape((rows, features), BF16),
        [picker, returned, *query_own],
        position,
    )
    *pieces, query_grad = lax.optimization_barrier((*pieces, query_grad))
    key_grad, value_grad = call(
        functools.partial(place_kernel, helpers),
        [shape((share, features), BF16)] * 2,
        pieces,
        position,
    )
    return query_grad[None], key_grad[None], value_grad[None]


def solution(mesh):
    split = P(None, ("ctx", "help"), None)
    shared = P(None, "ctx", None)

    return jax.shard_map(
        per_device,
        mesh=mesh,
        in_specs=(split, shared, shared, split, split),
        out_specs=(split, split, split),
        check_vma=False,
    )
```

```python
import functools

import jax
import jax.numpy as jnp
from jax import lax
from jax.experimental import pallas as pl
from jax.experimental.pallas import tpu as pltpu
from jax.sharding import PartitionSpec as P


HEAD_DIM = 128
CAPACITY = 8
NEGATIVE = -1e30
LOG2E = 1.4426950408889634
SCALING = HEAD_DIM ** (-0.5)
INFO = 16
TILE = 256
WIDE_TILE = 512
CHUNK = 64
VMEM_BYTES = 24 * 2**20
F32 = jnp.float32
BF16 = jnp.bfloat16


def iota(shape, dim):
    return lax.broadcasted_iota(jnp.int32, shape, dim)


def dot(a, b, ca, cb, precision=None):
    return lax.dot_general(
        a, b, (((ca,), (cb,)), ((), ())), precision=precision, preferred_element_type=F32
    )


def pack_kernel(blocks, helpers, pos, choice, query, grad, sent, picker_out, *own):
    rows = query.shape[0]
    width = query.shape[1] // helpers
    center = pos[0]
    helper = pos[1]
    slots = blocks * CAPACITY
    targets = []
    matches = []
    block_ids = iota((blocks, rows), 0)
    for r in range(2):
        c = choice[r : r + 1, :]
        t = jnp.where(c < center, center - 1 - c, -1)
        targets.append(t)
        matches.append(block_ids == t)
    counts = jnp.where(matches[0], 1.0, 0.0) + jnp.where(matches[1], 1.0, 0.0)
    before = jnp.where(iota((rows, rows), 0) < iota((rows, rows), 1), 1.0, 0.0).astype(BF16)
    earlier = dot(counts.astype(BF16), before, 1, 0)
    picker = jnp.zeros((slots, rows), F32)
    places = []
    for r in range(2):
        p = jnp.sum(jnp.where(matches[r], earlier, 0.0), axis=0, keepdims=True)
        places.append(p)
        code = jnp.where(targets[r] >= 0, targets[r] * CAPACITY + p.astype(jnp.int32), -1)
        picker = picker + jnp.where(iota((slots, rows), 0) == code, 1.0, 0.0)
    picker_out[...] = picker.T.astype(BF16)
    low = picker.astype(BF16)
    for d in range(helpers):
        for n, source in enumerate((query, grad)):
            got = dot(low, source[:, d * width : (d + 1) * width], 1, 0)
            sent[d, :, :, n * width : (n + 1) * width] = got.reshape(
                blocks, CAPACITY, width
            ).astype(BF16)
    info = jnp.concatenate([t.astype(F32) for t in targets] + places, axis=1)
    info = jnp.broadcast_to(info, (INFO, info.shape[1])).astype(BF16)
    for k in range(helpers):
        cols = pl.ds(pl.multiple_of((helper ^ k) * width, width), width)
        piece = piece_ref(own, k)
        piece[0:rows, 0:width] = query[:, cols]
        piece[0:rows, width : 2 * width] = grad[:, cols]
        piece[rows : rows + INFO, :] = info


def head_cols(head, heads, which):
    at = (which * heads + head) * HEAD_DIM
    return slice(at, at + HEAD_DIM)


def cols_of(head):
    return slice(head * HEAD_DIM, (head + 1) * HEAD_DIM)


def own_tile(own, helper, start, rows, cols):
    parts = [own[helper ^ g, 0:rows, cols] for g in range(start // rows, (start + TILE) // rows)]
    return jnp.concatenate(parts, axis=0)


def routed_tile(routed, tile, count, cols):
    helpers, _, capacity, _ = routed.shape
    group = helpers * capacity
    parts = [
        routed[:, tile * count + a, :, cols].astype(F32).reshape(group, HEAD_DIM)
        for a in range(count)
    ]
    return jnp.concatenate(parts, axis=0).astype(BF16)


def statistics_of(key, value, q, g, masked_from):
    scores = dot(key, q, 1, 1)
    products = dot(value, g, 1, 1)
    shape = (8, q.shape[0])
    highest = jnp.full(shape, NEGATIVE, F32)
    total = jnp.zeros(shape, F32)
    crossed = jnp.zeros(shape, F32)
    for at in range(0, key.shape[0], CHUNK):
        part = scores[at : at + CHUNK] * (SCALING * LOG2E)
        if masked_from is not None and at + CHUNK > masked_from:
            keep = iota(part.shape, 0) + (at - masked_from) <= iota(part.shape, 1)
            part = jnp.where(keep, part, NEGATIVE)
        part = part.reshape((CHUNK // 8,) + shape)
        newer = jnp.maximum(highest, jnp.max(part, axis=0))
        weights = jnp.exp2(part - newer)
        if masked_from is not None and at + CHUNK > masked_from:
            weights = jnp.where(keep.reshape(weights.shape), weights, 0.0)
        shrink = jnp.exp2(highest - newer)
        total = total * shrink + jnp.sum(weights, axis=0)
        crossed = crossed * shrink + jnp.sum(
            weights * products[at : at + CHUNK].reshape(part.shape), axis=0
        )
        highest = newer
    top = jnp.max(highest, axis=0, keepdims=True)
    shrink = jnp.exp2(highest - top)
    total = jnp.sum(total * shrink, axis=0, keepdims=True)
    crossed = jnp.sum(crossed * shrink, axis=0, keepdims=True)
    return top + jnp.log(total) * LOG2E, crossed / total


def own_statistics_kernel(heads, helpers, pos, own, key, value, out):
    helper = pos[1]
    rows = own.shape[1] - INFO
    length = key.shape[0]
    for head in range(heads):
        hc = cols_of(head)
        for start in range(0, length, TILE):
            end = start + TILE
            q = own_tile(own, helper, start, rows, head_cols(head, heads, 0))
            g = own_tile(own, helper, start, rows, head_cols(head, heads, 1))
            log_sum, mean = statistics_of(key[0:end, hc], value[0:end, hc], q, g, start)
            out[2 * head : 2 * head + 1, start:end] = log_sum
            out[2 * head + 1 : 2 * head + 2, start:end] = mean
    for n in range(4):
        parts = [
            own[helper ^ g, rows : rows + INFO, n * rows : (n + 1) * rows].astype(F32)[0:1]
            for g in range(helpers)
        ]
        out[2 * heads + n : 2 * heads + n + 1, :] = jnp.concatenate(parts, axis=1)


def routed_statistics_kernel(heads, routed, key, value, out):
    helpers, blocks, capacity, _ = routed.shape
    group = helpers * capacity
    count = TILE // group

    def body(tile, _):
        for head in range(heads):
            hc = cols_of(head)
            q = routed_tile(routed, tile, count, head_cols(head, heads, 0))
            g = routed_tile(routed, tile, count, head_cols(head, heads, 1))
            log_sum, mean = statistics_of(key[:, hc], value[:, hc], q, g, None)
            for a in range(count):
                cut = slice(a * group, (a + 1) * group)
                out[tile * count + a, head : head + 1, 0:group] = log_sum[:, cut]
                out[tile * count + a, head : head + 1, group : 2 * group] = mean[:, cut]
        return 0

    lax.fori_loop(0, blocks // count, body, 0)


def thirds(x, axis):
    high = x.astype(BF16)
    rest = x - high.astype(F32)
    middle = rest.astype(BF16)
    low = (rest - middle.astype(F32)).astype(BF16)
    return jnp.concatenate([high, middle, low], axis=axis)


def combine_kernel(heads, helpers, stats, got, totals, slots):
    length = stats.shape[1]
    blocks = got.shape[0]
    group = got.shape[2] // 2
    rows = length // helpers
    wide = 2 * group
    slot = iota((group, length), 0)
    in_group = (slot // CAPACITY) == (iota((group, length), 1) // rows)
    slot_place = (slot % CAPACITY).astype(F32)
    block_ids = iota((blocks, length), 0).astype(F32)
    hots = []
    masks = []
    present = []
    for r in range(2):
        t = stats[2 * heads + r : 2 * heads + r + 1, :]
        p = stats[2 * heads + 2 + r : 2 * heads + 3 + r, :]
        present.append(t >= 0.0)
        hots.append(jnp.where(block_ids == t, 1.0, 0.0).astype(BF16))
        masks.append(in_group & (slot_place == p) & (t >= 0.0))
    for head in range(heads):
        part = thirds(got[:, head, :].T, 1)
        logs = [stats[2 * head : 2 * head + 1, :]]
        means = [stats[2 * head + 1 : 2 * head + 2, :]]
        for r in range(2):
            hot = jnp.concatenate([hots[r]] * 3, axis=0)
            spread = dot(part, hot, 1, 0)
            log_r = jnp.sum(jnp.where(masks[r], spread[0:group], 0.0), axis=0, keepdims=True)
            mean_r = jnp.sum(jnp.where(masks[r], spread[group:wide], 0.0), axis=0, keepdims=True)
            logs.append(jnp.where(present[r], log_r, NEGATIVE))
            means.append(mean_r)
        top = jnp.maximum(jnp.maximum(logs[0], logs[1]), logs[2])
        shares = [jnp.exp2(v - top) for v in logs]
        norm = shares[0] + shares[1] + shares[2]
        log_total = top + jnp.log(norm) * LOG2E
        center = (shares[0] * means[0] + shares[1] * means[1] + shares[2] * means[2]) / norm
        totals[2 * head : 2 * head + 1, :] = log_total
        totals[2 * head + 1 : 2 * head + 2, :] = center
        logs3 = thirds(log_total, 0).astype(F32)
        means3 = thirds(center, 0).astype(F32)
        result = jnp.zeros((blocks, wide), F32)
        for r in range(2):
            for n in range(3):
                both = jnp.concatenate(
                    [
                        jnp.where(masks[r], logs3[n : n + 1], 0.0),
                        jnp.where(masks[r], means3[n : n + 1], 0.0),
                    ],
                    axis=0,
                ).astype(BF16)
                result = result + dot(hots[r], both, 1, 1)
        slots[:, head, :] = result


def mixed_into(mixed, probs, key, value, q, g, log_total, center, masked_from):
    scores = dot(key, q, 1, 1)
    products = dot(value, g, 1, 1)
    for at in range(0, key.shape[0], CHUNK):
        rows = slice(at, at + CHUNK)
        part = scores[rows] * (SCALING * LOG2E)
        if masked_from is not None and at + CHUNK > masked_from:
            keep = iota(part.shape, 0) + (at - masked_from) <= iota(part.shape, 1)
            part = jnp.where(keep, part, NEGATIVE)
        weights = jnp.exp2(part - log_total)
        if probs is not None:
            probs[rows, :] = weights.astype(BF16)
        mixed[rows, :] = (weights * (products[rows] - center)).astype(BF16)


def own_gradients_kernel(heads, pos, own, key, value, totals, key_out, value_out, *rest):
    *pieces, terms, mixed, probs = rest
    helper = pos[1]
    rows = own.shape[1] - INFO
    length = key.shape[0]
    for head in range(heads):
        hc = cols_of(head)
        turned = key[:, hc].T
        for start in reversed(range(0, length, TILE)):
            end = start + TILE
            q = own_tile(own, helper, start, rows, head_cols(head, heads, 0))
            g = own_tile(own, helper, start, rows, head_cols(head, heads, 1))
            log_total = totals[2 * head : 2 * head + 1, start:end]
            center = totals[2 * head + 1 : 2 * head + 2, start:end]
            mixed_into(
                mixed, probs, key[0:end, hc], value[0:end, hc], q, g, log_total, center, start
            )
            value_new = dot(g.T, probs[0:end, :], 1, 1)
            key_new = dot(q.T, mixed[0:end, :], 1, 1)
            if end == length:
                value_out[hc, :] = value_new
                key_out[hc, :] = key_new
            else:
                value_out[hc, 0:end] += value_new
                key_out[hc, 0:end] += key_new
            terms[start:end, hc] = (dot(turned[:, 0:end], mixed[0:end, :], 1, 0) * SCALING).T
    for k in range(length // rows):
        at = pl.ds(pl.multiple_of((helper ^ k) * rows, rows), rows)
        piece_ref(pieces, k)[...] = terms[at, :].astype(BF16)


def slot_row(slots, tile, count, head, which, group):
    cut = slice(which * group, (which + 1) * group)
    return jnp.concatenate(
        [slots[tile * count + a, head : head + 1, cut] for a in range(count)], axis=1
    )


def routed_gradients_kernel(
    heads, helpers, pos, routed, key, value, slots, key_own, value_own, out, *rest
):
    *pieces, key_acc, value_acc, key_got, value_got, staged, mixed, probs, sems = rest
    _, blocks, capacity, _ = routed.shape
    group = helpers * capacity
    count = WIDE_TILE // group
    steps = blocks // count
    key_copy = pltpu.make_async_copy(key_own, key_got, sems.at[0])
    value_copy = pltpu.make_async_copy(value_own, value_got, sems.at[1])
    key_copy.start()
    value_copy.start()
    turned = [key[:, cols_of(head)].T for head in range(heads)]

    def sending(tile):
        return pltpu.make_async_copy(
            staged.at[tile % 2],
            out.at[:, pl.ds(tile * count, count)],
            sems.at[2 + tile % 2],
        )

    key_acc[...] = jnp.zeros(key_acc.shape, F32)
    value_acc[...] = jnp.zeros(value_acc.shape, F32)

    def body(tile, _):
        slot = tile % 2

        @pl.when(tile >= 2)
        def _():
            sending(tile - 2).wait()

        for head in range(heads):
            hc = cols_of(head)
            q = routed_tile(routed, tile, count, head_cols(head, heads, 0))
            g = routed_tile(routed, tile, count, head_cols(head, heads, 1))
            log_total = slot_row(slots, tile, count, head, 0, group)
            center = slot_row(slots, tile, count, head, 1, group)
            low = mixed.at[head]
            high = probs.at[head]
            mixed_into(low, high, key[:, hc], value[:, hc], q, g, log_total, center, None)
            value_acc[hc, :] += dot(g.T, high[...], 1, 1)
            key_acc[hc, :] += dot(q.T, low[...], 1, 1)
            query_new = (dot(turned[head], low[...], 1, 0) * SCALING).T
            for a in range(count):
                staged[slot, :, a, :, hc] = (
                    query_new[a * group : (a + 1) * group]
                    .reshape(helpers, capacity, HEAD_DIM)
                    .astype(BF16)
                )
        sending(tile).start()
        return 0

    lax.fori_loop(0, steps, body, 0)
    key_copy.wait()
    value_copy.wait()
    width = key_acc.shape[0]
    share = key_acc.shape[1] // helpers
    for k in range(helpers):
        at = pl.ds(pl.multiple_of((pos[1] ^ k) * share, share), share)
        piece = piece_ref(pieces, k)
        piece[0:width, :] = ((key_acc[:, at] + key_got[:, at]) * SCALING).astype(BF16)
        piece[width : 2 * width, :] = (value_acc[:, at] + value_got[:, at]).astype(BF16)
    for tile in range(max(0, steps - 2), steps):
        sending(tile).wait()


def place_kernel(helpers, pos, *refs):
    pieces = refs[:helpers]
    key_out, value_out = refs[helpers:]
    width = key_out.shape[1] // helpers
    for k in range(helpers):
        cols = pl.ds(pl.multiple_of((pos[1] ^ k) * width, width), width)
        key_out[:, cols] = pieces[k][0:width, :].astype(F32).T.astype(BF16)
        value_out[:, cols] = pieces[k][width : 2 * width, :].astype(F32).T.astype(BF16)


def finish_kernel(helpers, pos, picker, returned, *refs):
    pieces = refs[:helpers]
    out = refs[helpers]
    width = out.shape[1] // helpers
    slots = picker.shape[1]
    for k in range(helpers):
        d = pos[1] ^ k
        cols = pl.ds(pl.multiple_of(d * width, width), width)
        terms = returned[d].astype(F32).reshape(slots, width).astype(BF16)
        out[:, cols] = (dot(picker[...], terms, 1, 0) + pieces[k][...].astype(F32)).astype(
            BF16
        )


DIRECT = (1, 3, 6)
RELAYED = ((2, 4, 6), (7, 5, 2))


def piece_shapes(shape, dtype, kind=pltpu.VMEM):
    one = kind(shape, dtype)
    pair = kind((2,) + shape, dtype)
    return [one] * (1 + len(DIRECT)) + [pair] * len(RELAYED)


def piece_ref(refs, k):
    if k == 0:
        return refs[0]
    if k in DIRECT:
        return refs[1 + DIRECT.index(k)]
    for n, (near, far, _) in enumerate(RELAYED):
        if k in (near, far):
            return refs[1 + len(DIRECT) + n].at[(near, far).index(k)]
    raise ValueError(k)


def exchange(pieces, helpers):
    def send(array, k):
        return lax.ppermute(array, "help", [(i, i ^ k) for i in range(helpers)])

    received = {0: pieces[0]}
    pairs = []
    for n, (near, _, _) in enumerate(RELAYED):
        pairs.append(send(pieces[1 + len(DIRECT) + n], near))
    for n, k in enumerate(DIRECT):
        received[k] = send(pieces[1 + n], k)
    for pair, (near, far, last) in zip(pairs, RELAYED):
        received[near] = pair[0]
        received[far] = send(pair[1], last)
    return [received[k] for k in range(helpers)]


def call(kernel, outputs, operands, position=None, scratch=(), flops=0, fast=99, hand_in=(), hand_out=()):
    vmem = pl.BlockSpec(memory_space=pltpu.VMEM)
    operands = [
        pltpu.with_memory_space_constraint(x, pltpu.VMEM if n < fast else pltpu.HBM)
        for n, x in enumerate(operands)
    ]
    hand = pl.BlockSpec(memory_space=pltpu.HBM)
    specs = [hand if n in hand_in else vmem for n in range(len(operands))]
    out_specs = None
    if hand_out:
        out_specs = [hand if n in hand_out else vmem for n in range(len(outputs))]
    if position is not None:
        operands = [position] + list(operands)
        specs = [pl.BlockSpec(memory_space=pltpu.SMEM)] + specs
    return pl.pallas_call(
        kernel,
        out_shape=outputs,
        in_specs=specs,
        **({"out_specs": out_specs} if out_specs else {}),
        scratch_shapes=scratch,
        compiler_params=pltpu.CompilerParams(vmem_limit_bytes=VMEM_BYTES),
        cost_estimate=pl.CostEstimate(flops=flops, bytes_accessed=0, transcendentals=0),
    )(*operands)


def swap(array, axes):
    return lax.all_to_all(array, axes, split_axis=0, concat_axis=0, tiled=True)


def per_device(query_rows, key_rows, value_rows, output_grad, block_choice):
    blocks = lax.axis_size("ctx")
    helpers = lax.axis_size("help")
    helper = lax.axis_index("help")
    position = jnp.stack([lax.axis_index("ctx"), helper]).astype(jnp.int32)
    _, rows, features = query_rows.shape
    length = key_rows.shape[1]
    width = features // helpers
    heads = width // HEAD_DIM
    group = helpers * CAPACITY
    slots = blocks * CAPACITY
    share = length // helpers
    pairs = 2 * blocks * group * length * width
    shape = jax.ShapeDtypeStruct
    fast = pltpu.VMEM
    everyone = ("help", "ctx")

    sent, picker, *pieces = call(
        functools.partial(pack_kernel, blocks, helpers),
        [pltpu.HBM((helpers, blocks, CAPACITY, 2 * width), BF16), shape((rows, slots), BF16)]
        + piece_shapes((rows + INFO, 2 * width), BF16),
        [jnp.transpose(block_choice[0]), query_rows[0], output_grad[0]],
        position,
        flops=2 * rows * slots * features * 2,
        fast=0,
    )
    own = jnp.stack(exchange(pieces, helpers))
    routed = swap(sent.reshape(blocks * helpers, CAPACITY, 2 * width), everyone)
    routed = routed.reshape(helpers, blocks, CAPACITY, 2 * width)

    key = lax.dynamic_slice_in_dim(key_rows[0], helper * width, width, 1)
    value = lax.dynamic_slice_in_dim(value_rows[0], helper * width, width, 1)
    stats = call(
        functools.partial(own_statistics_kernel, heads, helpers),
        fast((2 * heads + 4, length), F32),
        [own, key, value],
        position,
        flops=pairs // 2,
    )
    slot_shape = fast((blocks, heads, 2 * group), F32)
    parts = call(
        functools.partial(routed_statistics_kernel, heads),
        slot_shape,
        [routed, key, value],
        flops=2 * pairs,
    )
    parts = swap(parts, "ctx")

    totals, spread = call(
        functools.partial(combine_kernel, heads, helpers),
        [fast((2 * heads, length), F32), slot_shape],
        [stats, parts],
        flops=pairs // 8,
    )
    spread = swap(spread, "ctx")

    own_out = call(
        functools.partial(own_gradients_kernel, heads),
        [pltpu.HBM((width, length), F32)] * 2 + piece_shapes((rows, width), BF16, pltpu.HBM),
        [own, key, value, totals],
        position,
        [pltpu.VMEM((length, width), F32)] + [pltpu.VMEM((length, TILE), BF16)] * 2,
        flops=2 * pairs,
    )
    key_own, value_own, *query_own = own_out
    spread, key_own, value_own = lax.optimization_barrier((spread, key_own, value_own))
    query_own = exchange(query_own, helpers)

    terms, *pieces = call(
        functools.partial(routed_gradients_kernel, heads, helpers),
        [pltpu.HBM((helpers, blocks, CAPACITY, width), BF16)] + piece_shapes((2 * width, share), BF16, pltpu.HBM),
        [routed, key, value, spread, key_own, value_own],
        position,
        [pltpu.VMEM((width, length), F32)] * 4
        + [pltpu.VMEM((2, helpers, WIDE_TILE // group, CAPACITY, width), BF16)]
        + [pltpu.VMEM((heads, length, WIDE_TILE), BF16)] * 2
        + [pltpu.SemaphoreType.DMA((4,))],
        flops=5 * pairs,
        fast=4,
        hand_in=(4, 5),
        hand_out=(0,),
    )
    returned = swap(terms.reshape(blocks * helpers, CAPACITY, width), everyone)
    returned = returned.reshape(helpers, blocks, CAPACITY, width)

    pieces = exchange(pieces, helpers)

    query_grad = call(
        functools.partial(finish_kernel, helpers),
        shape((rows, features), BF16),
        [picker, returned, *query_own],
        position,
    )
    key_grad, value_grad = call(
        functools.partial(place_kernel, helpers),
        [shape((share, features), BF16)] * 2,
        pieces,
        position,
    )
    return query_grad[None], key_grad[None], value_grad[None]


def solution(mesh):
    split = P(None, ("ctx", "help"), None)
    shared = P(None, "ctx", None)

    return jax.shard_map(
        per_device,
        mesh=mesh,
        in_specs=(split, shared, shared, split, split),
        out_specs=(split, split, split),
        check_vma=False,
    )
```

```python
import functools

import jax
import jax.numpy as jnp
from jax import lax
from jax.experimental import pallas as pl
from jax.experimental.pallas import tpu as pltpu
from jax.sharding import PartitionSpec as P


HEAD_DIM = 128
CAPACITY = 8
NEGATIVE = -1e30
LOG2E = 1.4426950408889634
SCALING = HEAD_DIM ** (-0.5)
INFO = 16
TILE = 256
WIDE_TILE = 512
CHUNK = 64
VMEM_BYTES = 24 * 2**20
F32 = jnp.float32
BF16 = jnp.bfloat16


def iota(shape, dim):
    return lax.broadcasted_iota(jnp.int32, shape, dim)


def dot(a, b, ca, cb, precision=None):
    return lax.dot_general(
        a, b, (((ca,), (cb,)), ((), ())), precision=precision, preferred_element_type=F32
    )


def pack_kernel(
    blocks, helpers, pos, choice, query, grad, sent, picker_out, info_out, staged, sems
):
    rows = query.shape[0]
    width = query.shape[1] // helpers
    center = pos[0]
    slots = blocks * CAPACITY
    targets = []
    matches = []
    block_ids = iota((blocks, rows), 0)
    for r in range(2):
        c = choice[r : r + 1, :]
        t = jnp.where(c < center, center - 1 - c, -1)
        targets.append(t)
        matches.append(block_ids == t)
    counts = jnp.where(matches[0], 1.0, 0.0) + jnp.where(matches[1], 1.0, 0.0)
    before = jnp.where(iota((rows, rows), 0) < iota((rows, rows), 1), 1.0, 0.0).astype(BF16)
    earlier = dot(counts.astype(BF16), before, 1, 0)
    picker = jnp.zeros((slots, rows), F32)
    places = []
    for r in range(2):
        p = jnp.sum(jnp.where(matches[r], earlier, 0.0), axis=0, keepdims=True)
        places.append(p)
        code = jnp.where(targets[r] >= 0, targets[r] * CAPACITY + p.astype(jnp.int32), -1)
        picker = picker + jnp.where(iota((slots, rows), 0) == code, 1.0, 0.0)
    low = picker.astype(BF16)
    copies = []
    for d in range(helpers):
        for n, source in enumerate((query, grad)):
            got = dot(low, source[:, d * width : (d + 1) * width], 1, 0)
            staged[d, :, :, n * width : (n + 1) * width] = got.reshape(
                blocks, CAPACITY, width
            ).astype(BF16)
        copies.append(pltpu.make_async_copy(staged.at[d], sent.at[d], sems.at[d]))
        copies[-1].start()
    picker_out[...] = picker.T.astype(BF16)
    info = jnp.concatenate([t.astype(F32) for t in targets] + places, axis=1)
    info_out[...] = jnp.broadcast_to(info, (INFO, info.shape[1])).astype(BF16)
    for copy in copies:
        copy.wait()


def pack_own_kernel(helpers, pos, query, grad, info, *own):
    rows = query.shape[0]
    width = query.shape[1] // helpers
    for k in range(helpers):
        cols = pl.ds(pl.multiple_of((pos[1] ^ k) * width, width), width)
        piece = piece_ref(own, k)
        piece[0:rows, 0:width] = query[:, cols]
        piece[0:rows, width : 2 * width] = grad[:, cols]
        piece[rows : rows + INFO, :] = info[...]


def head_cols(head, heads, which):
    at = (which * heads + head) * HEAD_DIM
    return slice(at, at + HEAD_DIM)


def cols_of(head):
    return slice(head * HEAD_DIM, (head + 1) * HEAD_DIM)


def own_tile(own, helper, start, rows, cols):
    parts = [own[helper ^ g, 0:rows, cols] for g in range(start // rows, (start + TILE) // rows)]
    return jnp.concatenate(parts, axis=0)


def routed_tile(routed, tile, count, cols):
    helpers, _, capacity, _ = routed.shape
    group = helpers * capacity
    parts = [
        routed[:, tile * count + a, :, cols].astype(F32).reshape(group, HEAD_DIM)
        for a in range(count)
    ]
    return jnp.concatenate(parts, axis=0).astype(BF16)


def statistics_of(key, value, q, g, masked_from):
    scores = dot(key, q, 1, 1)
    products = dot(value, g, 1, 1)
    shape = (8, q.shape[0])
    highest = jnp.full(shape, NEGATIVE, F32)
    total = jnp.zeros(shape, F32)
    crossed = jnp.zeros(shape, F32)
    for at in range(0, key.shape[0], CHUNK):
        part = scores[at : at + CHUNK] * (SCALING * LOG2E)
        if masked_from is not None and at + CHUNK > masked_from:
            keep = iota(part.shape, 0) + (at - masked_from) <= iota(part.shape, 1)
            part = jnp.where(keep, part, NEGATIVE)
        part = part.reshape((CHUNK // 8,) + shape)
        newer = jnp.maximum(highest, jnp.max(part, axis=0))
        weights = jnp.exp2(part - newer)
        if masked_from is not None and at + CHUNK > masked_from:
            weights = jnp.where(keep.reshape(weights.shape), weights, 0.0)
        shrink = jnp.exp2(highest - newer)
        total = total * shrink + jnp.sum(weights, axis=0)
        crossed = crossed * shrink + jnp.sum(
            weights * products[at : at + CHUNK].reshape(part.shape), axis=0
        )
        highest = newer
    top = jnp.max(highest, axis=0, keepdims=True)
    shrink = jnp.exp2(highest - top)
    total = jnp.sum(total * shrink, axis=0, keepdims=True)
    crossed = jnp.sum(crossed * shrink, axis=0, keepdims=True)
    return top + jnp.log(total) * LOG2E, crossed / total


def own_statistics_kernel(heads, helpers, pos, own, key, value, out):
    helper = pos[1]
    rows = own.shape[1] - INFO
    length = key.shape[0]
    for head in range(heads):
        hc = cols_of(head)
        for start in range(0, length, TILE):
            end = start + TILE
            q = own_tile(own, helper, start, rows, head_cols(head, heads, 0))
            g = own_tile(own, helper, start, rows, head_cols(head, heads, 1))
            log_sum, mean = statistics_of(key[0:end, hc], value[0:end, hc], q, g, start)
            out[2 * head : 2 * head + 1, start:end] = log_sum
            out[2 * head + 1 : 2 * head + 2, start:end] = mean
    for n in range(4):
        parts = [
            own[helper ^ g, rows : rows + INFO, n * rows : (n + 1) * rows].astype(F32)[0:1]
            for g in range(helpers)
        ]
        out[2 * heads + n : 2 * heads + n + 1, :] = jnp.concatenate(parts, axis=1)


def routed_statistics_kernel(heads, routed, key, value, out):
    helpers, blocks, capacity, _ = routed.shape
    group = helpers * capacity
    count = TILE // group

    def body(tile, _):
        for head in range(heads):
            hc = cols_of(head)
            q = routed_tile(routed, tile, count, head_cols(head, heads, 0))
            g = routed_tile(routed, tile, count, head_cols(head, heads, 1))
            log_sum, mean = statistics_of(key[:, hc], value[:, hc], q, g, None)
            for a in range(count):
                cut = slice(a * group, (a + 1) * group)
                out[tile * count + a, head : head + 1, 0:group] = log_sum[:, cut]
                out[tile * count + a, head : head + 1, group : 2 * group] = mean[:, cut]
        return 0

    lax.fori_loop(0, blocks // count, body, 0)


def thirds(x, axis):
    high = x.astype(BF16)
    rest = x - high.astype(F32)
    middle = rest.astype(BF16)
    low = (rest - middle.astype(F32)).astype(BF16)
    return jnp.concatenate([high, middle, low], axis=axis)


def combine_kernel(heads, helpers, stats, got, totals, slots):
    length = stats.shape[1]
    blocks = got.shape[0]
    group = got.shape[2] // 2
    rows = length // helpers
    wide = 2 * group
    slot = iota((group, length), 0)
    in_group = (slot // CAPACITY) == (iota((group, length), 1) // rows)
    slot_place = (slot % CAPACITY).astype(F32)
    block_ids = iota((blocks, length), 0).astype(F32)
    hots = []
    masks = []
    present = []
    for r in range(2):
        t = stats[2 * heads + r : 2 * heads + r + 1, :]
        p = stats[2 * heads + 2 + r : 2 * heads + 3 + r, :]
        present.append(t >= 0.0)
        hots.append(jnp.where(block_ids == t, 1.0, 0.0).astype(BF16))
        masks.append(in_group & (slot_place == p) & (t >= 0.0))
    for head in range(heads):
        part = thirds(got[:, head, :].T, 1)
        logs = [stats[2 * head : 2 * head + 1, :]]
        means = [stats[2 * head + 1 : 2 * head + 2, :]]
        for r in range(2):
            hot = jnp.concatenate([hots[r]] * 3, axis=0)
            spread = dot(part, hot, 1, 0)
            log_r = jnp.sum(jnp.where(masks[r], spread[0:group], 0.0), axis=0, keepdims=True)
            mean_r = jnp.sum(jnp.where(masks[r], spread[group:wide], 0.0), axis=0, keepdims=True)
            logs.append(jnp.where(present[r], log_r, NEGATIVE))
            means.append(mean_r)
        top = jnp.maximum(jnp.maximum(logs[0], logs[1]), logs[2])
        shares = [jnp.exp2(v - top) for v in logs]
        norm = shares[0] + shares[1] + shares[2]
        log_total = top + jnp.log(norm) * LOG2E
        center = (shares[0] * means[0] + shares[1] * means[1] + shares[2] * means[2]) / norm
        totals[2 * head : 2 * head + 1, :] = log_total
        totals[2 * head + 1 : 2 * head + 2, :] = center
        logs3 = thirds(log_total, 0).astype(F32)
        means3 = thirds(center, 0).astype(F32)
        result = jnp.zeros((blocks, wide), F32)
        for r in range(2):
            for n in range(3):
                both = jnp.concatenate(
                    [
                        jnp.where(masks[r], logs3[n : n + 1], 0.0),
                        jnp.where(masks[r], means3[n : n + 1], 0.0),
                    ],
                    axis=0,
                ).astype(BF16)
                result = result + dot(hots[r], both, 1, 1)
        slots[:, head, :] = result


def mixed_into(mixed, probs, key, value, q, g, log_total, center, masked_from):
    scores = dot(key, q, 1, 1)
    products = dot(value, g, 1, 1)
    for at in range(0, key.shape[0], CHUNK):
        rows = slice(at, at + CHUNK)
        part = scores[rows] * (SCALING * LOG2E)
        if masked_from is not None and at + CHUNK > masked_from:
            keep = iota(part.shape, 0) + (at - masked_from) <= iota(part.shape, 1)
            part = jnp.where(keep, part, NEGATIVE)
        weights = jnp.exp2(part - log_total)
        if probs is not None:
            probs[rows, :] = weights.astype(BF16)
        mixed[rows, :] = (weights * (products[rows] - center)).astype(BF16)


def own_gradients_kernel(heads, pos, own, key, value, totals, key_out, value_out, *rest):
    *pieces, terms, mixed, probs = rest
    helper = pos[1]
    rows = own.shape[1] - INFO
    length = key.shape[0]
    for head in range(heads):
        hc = cols_of(head)
        turned = key[:, hc].T
        for start in reversed(range(0, length, TILE)):
            end = start + TILE
            q = own_tile(own, helper, start, rows, head_cols(head, heads, 0))
            g = own_tile(own, helper, start, rows, head_cols(head, heads, 1))
            log_total = totals[2 * head : 2 * head + 1, start:end]
            center = totals[2 * head + 1 : 2 * head + 2, start:end]
            mixed_into(
                mixed, probs, key[0:end, hc], value[0:end, hc], q, g, log_total, center, start
            )
            value_new = dot(g.T, probs[0:end, :], 1, 1)
            key_new = dot(q.T, mixed[0:end, :], 1, 1)
            if end == length:
                value_out[hc, :] = value_new
                key_out[hc, :] = key_new
            else:
                value_out[hc, 0:end] += value_new
                key_out[hc, 0:end] += key_new
            terms[start:end, hc] = (dot(turned[:, 0:end], mixed[0:end, :], 1, 0) * SCALING).T
    for k in range(length // rows):
        at = pl.ds(pl.multiple_of((helper ^ k) * rows, rows), rows)
        piece_ref(pieces, k)[...] = terms[at, :].astype(BF16)


def slot_row(slots, tile, count, head, which, group):
    cut = slice(which * group, (which + 1) * group)
    return jnp.concatenate(
        [slots[tile * count + a, head : head + 1, cut] for a in range(count)], axis=1
    )


def routed_gradients_kernel(
    heads, helpers, pos, routed, key, value, slots, key_own, value_own, out, *rest
):
    *pieces, key_acc, value_acc, key_got, value_got, staged, mixed, probs, sems = rest
    _, blocks, capacity, _ = routed.shape
    group = helpers * capacity
    count = WIDE_TILE // group
    steps = blocks // count
    key_copy = pltpu.make_async_copy(key_own, key_got, sems.at[0])
    value_copy = pltpu.make_async_copy(value_own, value_got, sems.at[1])
    key_copy.start()
    value_copy.start()
    turned = [key[:, cols_of(head)].T for head in range(heads)]

    def sending(tile):
        return pltpu.make_async_copy(
            staged.at[tile % 2],
            out.at[:, pl.ds(tile * count, count)],
            sems.at[2 + tile % 2],
        )

    key_acc[...] = jnp.zeros(key_acc.shape, F32)
    value_acc[...] = jnp.zeros(value_acc.shape, F32)

    def body(tile, _):
        slot = tile % 2

        @pl.when(tile >= 2)
        def _():
            sending(tile - 2).wait()

        for head in range(heads):
            hc = cols_of(head)
            q = routed_tile(routed, tile, count, head_cols(head, heads, 0))
            g = routed_tile(routed, tile, count, head_cols(head, heads, 1))
            log_total = slot_row(slots, tile, count, head, 0, group)
            center = slot_row(slots, tile, count, head, 1, group)
            low = mixed.at[head]
            high = probs.at[head]
            mixed_into(low, high, key[:, hc], value[:, hc], q, g, log_total, center, None)
            value_acc[hc, :] += dot(g.T, high[...], 1, 1)
            key_acc[hc, :] += dot(q.T, low[...], 1, 1)
            query_new = (dot(turned[head], low[...], 1, 0) * SCALING).T
            for a in range(count):
                staged[slot, :, a, :, hc] = (
                    query_new[a * group : (a + 1) * group]
                    .reshape(helpers, capacity, HEAD_DIM)
                    .astype(BF16)
                )
        sending(tile).start()
        return 0

    lax.fori_loop(0, steps, body, 0)
    key_copy.wait()
    value_copy.wait()
    width = key_acc.shape[0]
    share = key_acc.shape[1] // helpers
    for k in range(helpers):
        at = pl.ds(pl.multiple_of((pos[1] ^ k) * share, share), share)
        piece = piece_ref(pieces, k)
        piece[0:width, :] = ((key_acc[:, at] + key_got[:, at]) * SCALING).astype(BF16)
        piece[width : 2 * width, :] = (value_acc[:, at] + value_got[:, at]).astype(BF16)
    for tile in range(max(0, steps - 2), steps):
        sending(tile).wait()


def place_kernel(helpers, pos, *refs):
    pieces = refs[:helpers]
    key_out, value_out = refs[helpers:]
    width = key_out.shape[1] // helpers
    for k in range(helpers):
        cols = pl.ds(pl.multiple_of((pos[1] ^ k) * width, width), width)
        key_out[:, cols] = pieces[k][0:width, :].astype(F32).T.astype(BF16)
        value_out[:, cols] = pieces[k][width : 2 * width, :].astype(F32).T.astype(BF16)


def finish_kernel(helpers, pos, picker, returned, *refs):
    pieces = refs[:helpers]
    out = refs[helpers]
    width = out.shape[1] // helpers
    slots = picker.shape[1]
    for k in range(helpers):
        d = pos[1] ^ k
        cols = pl.ds(pl.multiple_of(d * width, width), width)
        terms = returned[d].astype(F32).reshape(slots, width).astype(BF16)
        out[:, cols] = (dot(picker[...], terms, 1, 0) + pieces[k][...].astype(F32)).astype(
            BF16
        )


DIRECT = (1, 3, 6)
RELAYED = ((2, 4, 6), (7, 5, 2))


def piece_shapes(shape, dtype, kind=pltpu.VMEM):
    one = kind(shape, dtype)
    pair = kind((2,) + shape, dtype)
    return [one] * (1 + len(DIRECT)) + [pair] * len(RELAYED)


def piece_ref(refs, k):
    if k == 0:
        return refs[0]
    if k in DIRECT:
        return refs[1 + DIRECT.index(k)]
    for n, (near, far, _) in enumerate(RELAYED):
        if k in (near, far):
            return refs[1 + len(DIRECT) + n].at[(near, far).index(k)]
    raise ValueError(k)


def exchange(pieces, helpers):
    def send(array, k):
        return lax.ppermute(array, "help", [(i, i ^ k) for i in range(helpers)])

    received = {0: pieces[0]}
    pairs = []
    for n, (near, _, _) in enumerate(RELAYED):
        pairs.append(send(pieces[1 + len(DIRECT) + n], near))
    for n, k in enumerate(DIRECT):
        received[k] = send(pieces[1 + n], k)
    for pair, (near, far, last) in zip(pairs, RELAYED):
        received[near] = pair[0]
        received[far] = send(pair[1], last)
    return [received[k] for k in range(helpers)]


def call(kernel, outputs, operands, position=None, scratch=(), flops=0, fast=99, hand_in=(), hand_out=()):
    vmem = pl.BlockSpec(memory_space=pltpu.VMEM)
    operands = [
        pltpu.with_memory_space_constraint(x, pltpu.VMEM if n < fast else pltpu.HBM)
        for n, x in enumerate(operands)
    ]
    hand = pl.BlockSpec(memory_space=pltpu.HBM)
    specs = [hand if n in hand_in else vmem for n in range(len(operands))]
    out_specs = None
    if hand_out:
        out_specs = [hand if n in hand_out else vmem for n in range(len(outputs))]
    if position is not None:
        operands = [position] + list(operands)
        specs = [pl.BlockSpec(memory_space=pltpu.SMEM)] + specs
    return pl.pallas_call(
        kernel,
        out_shape=outputs,
        in_specs=specs,
        **({"out_specs": out_specs} if out_specs else {}),
        scratch_shapes=scratch,
        compiler_params=pltpu.CompilerParams(vmem_limit_bytes=VMEM_BYTES),
        cost_estimate=pl.CostEstimate(flops=flops, bytes_accessed=0, transcendentals=0),
    )(*operands)


def swap(array, axes):
    return lax.all_to_all(array, axes, split_axis=0, concat_axis=0, tiled=True)


def per_device(query_rows, key_rows, value_rows, output_grad, block_choice):
    blocks = lax.axis_size("ctx")
    helpers = lax.axis_size("help")
    helper = lax.axis_index("help")
    position = jnp.stack([lax.axis_index("ctx"), helper]).astype(jnp.int32)
    _, rows, features = query_rows.shape
    length = key_rows.shape[1]
    width = features // helpers
    heads = width // HEAD_DIM
    group = helpers * CAPACITY
    slots = blocks * CAPACITY
    share = length // helpers
    pairs = 2 * blocks * group * length * width
    shape = jax.ShapeDtypeStruct
    fast = pltpu.VMEM
    everyone = ("help", "ctx")

    sent, picker, info = call(
        functools.partial(pack_kernel, blocks, helpers),
        [
            pltpu.HBM((helpers, blocks, CAPACITY, 2 * width), BF16),
            pltpu.HBM((rows, slots), BF16),
            pltpu.HBM((INFO, 2 * width), BF16),
        ],
        [jnp.transpose(block_choice[0]), query_rows[0], output_grad[0]],
        position,
        [
            pltpu.VMEM((helpers, blocks, CAPACITY, 2 * width), BF16),
            pltpu.SemaphoreType.DMA((helpers,)),
        ],
        flops=2 * rows * slots * features * 2,
        fast=0,
        hand_out=(0,),
    )
    pieces = call(
        functools.partial(pack_own_kernel, helpers),
        piece_shapes((rows + INFO, 2 * width), BF16, pltpu.HBM),
        [query_rows[0], output_grad[0], info],
        position,
        fast=0,
    )
    own = jnp.stack(exchange(pieces, helpers))
    routed = swap(sent.reshape(blocks * helpers, CAPACITY, 2 * width), everyone)
    routed = routed.reshape(helpers, blocks, CAPACITY, 2 * width)

    key = lax.dynamic_slice_in_dim(key_rows[0], helper * width, width, 1)
    value = lax.dynamic_slice_in_dim(value_rows[0], helper * width, width, 1)
    stats = call(
        functools.partial(own_statistics_kernel, heads, helpers),
        fast((2 * heads + 4, length), F32),
        [own, key, value],
        position,
        flops=pairs // 2,
    )
    slot_shape = fast((blocks, heads, 2 * group), F32)
    parts = call(
        functools.partial(routed_statistics_kernel, heads),
        slot_shape,
        [routed, key, value],
        flops=2 * pairs,
    )
    parts = swap(parts, "ctx")

    totals, spread = call(
        functools.partial(combine_kernel, heads, helpers),
        [fast((2 * heads, length), F32), slot_shape],
        [stats, parts],
        flops=pairs // 8,
    )
    spread = swap(spread, "ctx")

    own_out = call(
        functools.partial(own_gradients_kernel, heads),
        [pltpu.HBM((width, length), F32)] * 2 + piece_shapes((rows, width), BF16, pltpu.HBM),
        [own, key, value, totals],
        position,
        [pltpu.VMEM((length, width), F32)] + [pltpu.VMEM((length, TILE), BF16)] * 2,
        flops=2 * pairs,
    )
    key_own, value_own, *query_own = own_out
    spread, key_own, value_own = lax.optimization_barrier((spread, key_own, value_own))
    query_own = exchange(query_own, helpers)

    terms, *pieces = call(
        functools.partial(routed_gradients_kernel, heads, helpers),
        [pltpu.HBM((helpers, blocks, CAPACITY, width), BF16)] + piece_shapes((2 * width, share), BF16, pltpu.HBM),
        [routed, key, value, spread, key_own, value_own],
        position,
        [pltpu.VMEM((width, length), F32)] * 4
        + [pltpu.VMEM((2, helpers, WIDE_TILE // group, CAPACITY, width), BF16)]
        + [pltpu.VMEM((heads, length, WIDE_TILE), BF16)] * 2
        + [pltpu.SemaphoreType.DMA((4,))],
        flops=5 * pairs,
        fast=4,
        hand_in=(4, 5),
        hand_out=(0,),
    )
    returned = swap(terms.reshape(blocks * helpers, CAPACITY, width), everyone)
    returned = returned.reshape(helpers, blocks, CAPACITY, width)

    pieces = exchange(pieces, helpers)

    query_grad = call(
        functools.partial(finish_kernel, helpers),
        shape((rows, features), BF16),
        [picker, returned, *query_own],
        position,
    )
    key_grad, value_grad = call(
        functools.partial(place_kernel, helpers),
        [shape((share, features), BF16)] * 2,
        pieces,
        position,
    )
    return query_grad[None], key_grad[None], value_grad[None]


def solution(mesh):
    split = P(None, ("ctx", "help"), None)
    shared = P(None, "ctx", None)

    return jax.shard_map(
        per_device,
        mesh=mesh,
        in_specs=(split, shared, shared, split, split),
        out_specs=(split, split, split),
        check_vma=False,
    )
```

```python
import functools

import jax
import jax.numpy as jnp
from jax import lax
from jax.experimental import pallas as pl
from jax.experimental.pallas import tpu as pltpu
from jax.sharding import PartitionSpec as P


HEAD_DIM = 128
CAPACITY = 8
NEGATIVE = -1e30
LOG2E = 1.4426950408889634
SCALING = HEAD_DIM ** (-0.5)
INFO = 16
TILE = 256
WIDE_TILE = 512
CHUNK = 64
VMEM_BYTES = 24 * 2**20
F32 = jnp.float32
BF16 = jnp.bfloat16


def iota(shape, dim):
    return lax.broadcasted_iota(jnp.int32, shape, dim)


def dot(a, b, ca, cb, precision=None):
    return lax.dot_general(
        a, b, (((ca,), (cb,)), ((), ())), precision=precision, preferred_element_type=F32
    )


def pack_kernel(
    blocks, helpers, pos, choice, query, grad, sent, picker_out, info_out, staged, sems
):
    rows = query.shape[0]
    width = query.shape[1] // helpers
    center = pos[0]
    slots = blocks * CAPACITY
    targets = []
    matches = []
    block_ids = iota((blocks, rows), 0)
    for r in range(2):
        c = choice[r : r + 1, :]
        t = jnp.where(c < center, center - 1 - c, -1)
        targets.append(t)
        matches.append(block_ids == t)
    counts = jnp.where(matches[0], 1.0, 0.0) + jnp.where(matches[1], 1.0, 0.0)
    before = jnp.where(iota((rows, rows), 0) < iota((rows, rows), 1), 1.0, 0.0).astype(BF16)
    earlier = dot(counts.astype(BF16), before, 1, 0)
    picker = jnp.zeros((slots, rows), F32)
    places = []
    for r in range(2):
        p = jnp.sum(jnp.where(matches[r], earlier, 0.0), axis=0, keepdims=True)
        places.append(p)
        code = jnp.where(targets[r] >= 0, targets[r] * CAPACITY + p.astype(jnp.int32), -1)
        picker = picker + jnp.where(iota((slots, rows), 0) == code, 1.0, 0.0)
    low = picker.astype(BF16)
    copies = []
    for d in range(helpers):
        for n, source in enumerate((query, grad)):
            got = dot(low, source[:, d * width : (d + 1) * width], 1, 0)
            staged[d, :, :, n * width : (n + 1) * width] = got.reshape(
                blocks, CAPACITY, width
            ).astype(BF16)
        copies.append(pltpu.make_async_copy(staged.at[d], sent.at[d], sems.at[d]))
        copies[-1].start()
    picker_out[...] = picker.T.astype(BF16)
    info = jnp.concatenate([t.astype(F32) for t in targets] + places, axis=1)
    info_out[...] = jnp.broadcast_to(info, (INFO, info.shape[1])).astype(BF16)
    for copy in copies:
        copy.wait()


def pack_own_kernel(helpers, pos, query, grad, info, *own):
    rows = query.shape[0]
    width = query.shape[1] // helpers
    for k in range(helpers):
        cols = pl.ds(pl.multiple_of((pos[1] ^ k) * width, width), width)
        piece = piece_ref(own, k)
        piece[0:rows, 0:width] = query[:, cols]
        piece[0:rows, width : 2 * width] = grad[:, cols]
        piece[rows : rows + INFO, :] = info[...]


def head_cols(head, heads, which):
    at = (which * heads + head) * HEAD_DIM
    return slice(at, at + HEAD_DIM)


def cols_of(head):
    return slice(head * HEAD_DIM, (head + 1) * HEAD_DIM)


def own_tile(own, helper, start, rows, cols):
    parts = [own[helper ^ g, 0:rows, cols] for g in range(start // rows, (start + TILE) // rows)]
    return jnp.concatenate(parts, axis=0)


def routed_tile(routed, tile, count, cols):
    helpers, _, capacity, _ = routed.shape
    group = helpers * capacity
    parts = [
        routed[:, tile * count + a, :, cols].astype(F32).reshape(group, HEAD_DIM)
        for a in range(count)
    ]
    return jnp.concatenate(parts, axis=0).astype(BF16)


def statistics_of(key, value, q, g, masked_from):
    scores = dot(key, q, 1, 1)
    products = dot(value, g, 1, 1)
    shape = (8, q.shape[0])
    highest = jnp.full(shape, NEGATIVE, F32)
    total = jnp.zeros(shape, F32)
    crossed = jnp.zeros(shape, F32)
    for at in range(0, key.shape[0], CHUNK):
        part = scores[at : at + CHUNK] * (SCALING * LOG2E)
        if masked_from is not None and at + CHUNK > masked_from:
            keep = iota(part.shape, 0) + (at - masked_from) <= iota(part.shape, 1)
            part = jnp.where(keep, part, NEGATIVE)
        part = part.reshape((CHUNK // 8,) + shape)
        newer = jnp.maximum(highest, jnp.max(part, axis=0))
        weights = jnp.exp2(part - newer)
        if masked_from is not None and at + CHUNK > masked_from:
            weights = jnp.where(keep.reshape(weights.shape), weights, 0.0)
        shrink = jnp.exp2(highest - newer)
        total = total * shrink + jnp.sum(weights, axis=0)
        crossed = crossed * shrink + jnp.sum(
            weights * products[at : at + CHUNK].reshape(part.shape), axis=0
        )
        highest = newer
    top = jnp.max(highest, axis=0, keepdims=True)
    shrink = jnp.exp2(highest - top)
    total = jnp.sum(total * shrink, axis=0, keepdims=True)
    crossed = jnp.sum(crossed * shrink, axis=0, keepdims=True)
    return top + jnp.log(total) * LOG2E, crossed / total


def own_statistics_kernel(heads, helpers, pos, own, key, value, out):
    helper = pos[1]
    rows = own.shape[1] - INFO
    length = key.shape[0]
    for head in range(heads):
        hc = cols_of(head)
        for start in range(0, length, TILE):
            end = start + TILE
            q = own_tile(own, helper, start, rows, head_cols(head, heads, 0))
            g = own_tile(own, helper, start, rows, head_cols(head, heads, 1))
            log_sum, mean = statistics_of(key[0:end, hc], value[0:end, hc], q, g, start)
            out[2 * head : 2 * head + 1, start:end] = log_sum
            out[2 * head + 1 : 2 * head + 2, start:end] = mean
    for n in range(4):
        parts = [
            own[helper ^ g, rows : rows + INFO, n * rows : (n + 1) * rows].astype(F32)[0:1]
            for g in range(helpers)
        ]
        out[2 * heads + n : 2 * heads + n + 1, :] = jnp.concatenate(parts, axis=1)


def routed_statistics_kernel(heads, routed, key, value, out):
    helpers, blocks, capacity, _ = routed.shape
    group = helpers * capacity
    count = TILE // group

    def body(tile, _):
        for head in range(heads):
            hc = cols_of(head)
            q = routed_tile(routed, tile, count, head_cols(head, heads, 0))
            g = routed_tile(routed, tile, count, head_cols(head, heads, 1))
            log_sum, mean = statistics_of(key[:, hc], value[:, hc], q, g, None)
            for a in range(count):
                cut = slice(a * group, (a + 1) * group)
                out[tile * count + a, head : head + 1, 0:group] = log_sum[:, cut]
                out[tile * count + a, head : head + 1, group : 2 * group] = mean[:, cut]
        return 0

    lax.fori_loop(0, blocks // count, body, 0)


def thirds(x, axis):
    high = x.astype(BF16)
    rest = x - high.astype(F32)
    middle = rest.astype(BF16)
    low = (rest - middle.astype(F32)).astype(BF16)
    return jnp.concatenate([high, middle, low], axis=axis)


def combine_kernel(heads, helpers, stats, got, totals, slots):
    length = stats.shape[1]
    blocks = got.shape[0]
    group = got.shape[2] // 2
    rows = length // helpers
    wide = 2 * group
    slot = iota((group, length), 0)
    in_group = (slot // CAPACITY) == (iota((group, length), 1) // rows)
    slot_place = (slot % CAPACITY).astype(F32)
    block_ids = iota((blocks, length), 0).astype(F32)
    hots = []
    masks = []
    present = []
    for r in range(2):
        t = stats[2 * heads + r : 2 * heads + r + 1, :]
        p = stats[2 * heads + 2 + r : 2 * heads + 3 + r, :]
        present.append(t >= 0.0)
        hots.append(jnp.where(block_ids == t, 1.0, 0.0).astype(BF16))
        masks.append(in_group & (slot_place == p) & (t >= 0.0))
    for head in range(heads):
        part = thirds(got[:, head, :].T, 1)
        logs = [stats[2 * head : 2 * head + 1, :]]
        means = [stats[2 * head + 1 : 2 * head + 2, :]]
        for r in range(2):
            hot = jnp.concatenate([hots[r]] * 3, axis=0)
            spread = dot(part, hot, 1, 0)
            log_r = jnp.sum(jnp.where(masks[r], spread[0:group], 0.0), axis=0, keepdims=True)
            mean_r = jnp.sum(jnp.where(masks[r], spread[group:wide], 0.0), axis=0, keepdims=True)
            logs.append(jnp.where(present[r], log_r, NEGATIVE))
            means.append(mean_r)
        top = jnp.maximum(jnp.maximum(logs[0], logs[1]), logs[2])
        shares = [jnp.exp2(v - top) for v in logs]
        norm = shares[0] + shares[1] + shares[2]
        log_total = top + jnp.log(norm) * LOG2E
        center = (shares[0] * means[0] + shares[1] * means[1] + shares[2] * means[2]) / norm
        totals[2 * head : 2 * head + 1, :] = log_total
        totals[2 * head + 1 : 2 * head + 2, :] = center
        logs3 = thirds(log_total, 0).astype(F32)
        means3 = thirds(center, 0).astype(F32)
        result = jnp.zeros((blocks, wide), F32)
        for r in range(2):
            for n in range(3):
                both = jnp.concatenate(
                    [
                        jnp.where(masks[r], logs3[n : n + 1], 0.0),
                        jnp.where(masks[r], means3[n : n + 1], 0.0),
                    ],
                    axis=0,
                ).astype(BF16)
                result = result + dot(hots[r], both, 1, 1)
        slots[:, head, :] = result


def mixed_into(mixed, probs, key, value, q, g, log_total, center, masked_from):
    scores = dot(key, q, 1, 1)
    products = dot(value, g, 1, 1)
    for at in range(0, key.shape[0], CHUNK):
        rows = slice(at, at + CHUNK)
        part = scores[rows] * (SCALING * LOG2E)
        if masked_from is not None and at + CHUNK > masked_from:
            keep = iota(part.shape, 0) + (at - masked_from) <= iota(part.shape, 1)
            part = jnp.where(keep, part, NEGATIVE)
        weights = jnp.exp2(part - log_total)
        if probs is not None:
            probs[rows, :] = weights.astype(BF16)
        mixed[rows, :] = (weights * (products[rows] - center)).astype(BF16)


def own_gradients_kernel(heads, pos, own, key, value, totals, key_out, value_out, *rest):
    *pieces, terms, mixed, probs = rest
    helper = pos[1]
    rows = own.shape[1] - INFO
    length = key.shape[0]
    for head in range(heads):
        hc = cols_of(head)
        turned = key[:, hc].T
        for start in reversed(range(0, length, TILE)):
            end = start + TILE
            q = own_tile(own, helper, start, rows, head_cols(head, heads, 0))
            g = own_tile(own, helper, start, rows, head_cols(head, heads, 1))
            log_total = totals[2 * head : 2 * head + 1, start:end]
            center = totals[2 * head + 1 : 2 * head + 2, start:end]
            mixed_into(
                mixed, probs, key[0:end, hc], value[0:end, hc], q, g, log_total, center, start
            )
            value_new = dot(g.T, probs[0:end, :], 1, 1)
            key_new = dot(q.T, mixed[0:end, :], 1, 1)
            if end == length:
                value_out[hc, :] = value_new
                key_out[hc, :] = key_new
            else:
                value_out[hc, 0:end] += value_new
                key_out[hc, 0:end] += key_new
            terms[start:end, hc] = (dot(turned[:, 0:end], mixed[0:end, :], 1, 0) * SCALING).T
    for k in range(length // rows):
        at = pl.ds(pl.multiple_of((helper ^ k) * rows, rows), rows)
        piece_ref(pieces, k)[...] = terms[at, :].astype(BF16)


def slot_row(slots, tile, count, head, which, group):
    cut = slice(which * group, (which + 1) * group)
    return jnp.concatenate(
        [slots[tile * count + a, head : head + 1, cut] for a in range(count)], axis=1
    )


def routed_gradients_kernel(
    heads, helpers, pos, routed, key, value, slots, key_own, value_own, out, *rest
):
    *pieces, key_acc, value_acc, key_got, value_got, staged, mixed, probs, sems = rest
    _, blocks, capacity, _ = routed.shape
    group = helpers * capacity
    count = WIDE_TILE // group
    steps = blocks // count
    key_copy = pltpu.make_async_copy(key_own, key_got, sems.at[0])
    value_copy = pltpu.make_async_copy(value_own, value_got, sems.at[1])
    key_copy.start()
    value_copy.start()
    turned = [key[:, cols_of(head)].T for head in range(heads)]

    def sending(tile):
        return pltpu.make_async_copy(
            staged.at[tile % 2],
            out.at[:, pl.ds(tile * count, count)],
            sems.at[2 + tile % 2],
        )

    key_acc[...] = jnp.zeros(key_acc.shape, F32)
    value_acc[...] = jnp.zeros(value_acc.shape, F32)

    def body(tile, _):
        slot = tile % 2

        @pl.when(tile >= 2)
        def _():
            sending(tile - 2).wait()

        for head in range(heads):
            hc = cols_of(head)
            q = routed_tile(routed, tile, count, head_cols(head, heads, 0))
            g = routed_tile(routed, tile, count, head_cols(head, heads, 1))
            log_total = slot_row(slots, tile, count, head, 0, group)
            center = slot_row(slots, tile, count, head, 1, group)
            low = mixed.at[head]
            high = probs.at[head]
            mixed_into(low, high, key[:, hc], value[:, hc], q, g, log_total, center, None)
            value_acc[hc, :] += dot(g.T, high[...], 1, 1)
            key_acc[hc, :] += dot(q.T, low[...], 1, 1)
            query_new = (dot(turned[head], low[...], 1, 0) * SCALING).T
            for a in range(count):
                staged[slot, :, a, :, hc] = (
                    query_new[a * group : (a + 1) * group]
                    .reshape(helpers, capacity, HEAD_DIM)
                    .astype(BF16)
                )
        sending(tile).start()
        return 0

    lax.fori_loop(0, steps, body, 0)
    key_copy.wait()
    value_copy.wait()
    width = key_acc.shape[0]
    share = key_acc.shape[1] // helpers
    for k in range(helpers):
        at = pl.ds(pl.multiple_of((pos[1] ^ k) * share, share), share)
        piece = piece_ref(pieces, k)
        piece[0:width, :] = ((key_acc[:, at] + key_got[:, at]) * SCALING).astype(BF16)
        piece[width : 2 * width, :] = (value_acc[:, at] + value_got[:, at]).astype(BF16)
    for tile in range(max(0, steps - 2), steps):
        sending(tile).wait()


def place_kernel(helpers, pos, *refs):
    pieces = refs[:helpers]
    key_out, value_out = refs[helpers:]
    width = key_out.shape[1] // helpers
    for k in range(helpers):
        cols = pl.ds(pl.multiple_of((pos[1] ^ k) * width, width), width)
        key_out[:, cols] = pieces[k][0:width, :].astype(F32).T.astype(BF16)
        value_out[:, cols] = pieces[k][width : 2 * width, :].astype(F32).T.astype(BF16)


def finish_kernel(helpers, pos, picker, returned, *refs):
    *pieces, out, staged, sems = refs
    width = out.shape[1] // helpers
    slots = picker.shape[1]
    copies = []
    for k in range(helpers):
        d = pos[1] ^ k
        cols = pl.ds(pl.multiple_of(d * width, width), width)
        terms = returned[d].astype(F32).reshape(slots, width).astype(BF16)
        total = dot(picker[...], terms, 1, 0) + pieces[k][...].astype(F32)
        staged[k] = total.astype(BF16)
        copies.append(pltpu.make_async_copy(staged.at[k], out.at[:, cols], sems.at[k]))
        copies[-1].start()
    for copy in copies:
        copy.wait()


DIRECT = (1, 3, 6)
RELAYED = ((2, 4, 6), (7, 5, 2))


def piece_shapes(shape, dtype, kind=pltpu.VMEM):
    one = kind(shape, dtype)
    pair = kind((2,) + shape, dtype)
    return [one] * (1 + len(DIRECT)) + [pair] * len(RELAYED)


def piece_ref(refs, k):
    if k == 0:
        return refs[0]
    if k in DIRECT:
        return refs[1 + DIRECT.index(k)]
    for n, (near, far, _) in enumerate(RELAYED):
        if k in (near, far):
            return refs[1 + len(DIRECT) + n].at[(near, far).index(k)]
    raise ValueError(k)


def exchange(pieces, helpers):
    def send(array, k):
        return lax.ppermute(array, "help", [(i, i ^ k) for i in range(helpers)])

    received = {0: pieces[0]}
    pairs = []
    for n, (near, _, _) in enumerate(RELAYED):
        pairs.append(send(pieces[1 + len(DIRECT) + n], near))
    for n, k in enumerate(DIRECT):
        received[k] = send(pieces[1 + n], k)
    for pair, (near, far, last) in zip(pairs, RELAYED):
        received[near] = pair[0]
        received[far] = send(pair[1], last)
    return [received[k] for k in range(helpers)]


def call(kernel, outputs, operands, position=None, scratch=(), flops=0, fast=99, hand_in=(), hand_out=()):
    vmem = pl.BlockSpec(memory_space=pltpu.VMEM)
    operands = [
        pltpu.with_memory_space_constraint(x, pltpu.VMEM if n < fast else pltpu.HBM)
        for n, x in enumerate(operands)
    ]
    hand = pl.BlockSpec(memory_space=pltpu.HBM)
    specs = [hand if n in hand_in else vmem for n in range(len(operands))]
    out_specs = None
    if hand_out:
        out_specs = [hand if n in hand_out else vmem for n in range(len(outputs))]
    if position is not None:
        operands = [position] + list(operands)
        specs = [pl.BlockSpec(memory_space=pltpu.SMEM)] + specs
    return pl.pallas_call(
        kernel,
        out_shape=outputs,
        in_specs=specs,
        **({"out_specs": out_specs} if out_specs else {}),
        scratch_shapes=scratch,
        compiler_params=pltpu.CompilerParams(vmem_limit_bytes=VMEM_BYTES),
        cost_estimate=pl.CostEstimate(flops=flops, bytes_accessed=0, transcendentals=0),
    )(*operands)


def swap(array, axes):
    return lax.all_to_all(array, axes, split_axis=0, concat_axis=0, tiled=True)


def per_device(query_rows, key_rows, value_rows, output_grad, block_choice):
    blocks = lax.axis_size("ctx")
    helpers = lax.axis_size("help")
    helper = lax.axis_index("help")
    position = jnp.stack([lax.axis_index("ctx"), helper]).astype(jnp.int32)
    _, rows, features = query_rows.shape
    length = key_rows.shape[1]
    width = features // helpers
    heads = width // HEAD_DIM
    group = helpers * CAPACITY
    slots = blocks * CAPACITY
    share = length // helpers
    pairs = 2 * blocks * group * length * width
    shape = jax.ShapeDtypeStruct
    fast = pltpu.VMEM
    everyone = ("help", "ctx")

    sent, picker, info = call(
        functools.partial(pack_kernel, blocks, helpers),
        [
            pltpu.HBM((helpers, blocks, CAPACITY, 2 * width), BF16),
            pltpu.HBM((rows, slots), BF16),
            pltpu.HBM((INFO, 2 * width), BF16),
        ],
        [jnp.transpose(block_choice[0]), query_rows[0], output_grad[0]],
        position,
        [
            pltpu.VMEM((helpers, blocks, CAPACITY, 2 * width), BF16),
            pltpu.SemaphoreType.DMA((helpers,)),
        ],
        flops=2 * rows * slots * features * 2,
        fast=0,
        hand_out=(0,),
    )
    pieces = call(
        functools.partial(pack_own_kernel, helpers),
        piece_shapes((rows + INFO, 2 * width), BF16, pltpu.HBM),
        [query_rows[0], output_grad[0], info],
        position,
        fast=0,
    )
    own = jnp.stack(exchange(pieces, helpers))
    routed = swap(sent.reshape(blocks * helpers, CAPACITY, 2 * width), everyone)
    routed = routed.reshape(helpers, blocks, CAPACITY, 2 * width)

    key = lax.dynamic_slice_in_dim(key_rows[0], helper * width, width, 1)
    value = lax.dynamic_slice_in_dim(value_rows[0], helper * width, width, 1)
    stats = call(
        functools.partial(own_statistics_kernel, heads, helpers),
        fast((2 * heads + 4, length), F32),
        [own, key, value],
        position,
        flops=pairs // 2,
    )
    slot_shape = fast((blocks, heads, 2 * group), F32)
    parts = call(
        functools.partial(routed_statistics_kernel, heads),
        slot_shape,
        [routed, key, value],
        flops=2 * pairs,
    )
    parts = swap(parts, "ctx")

    totals, spread = call(
        functools.partial(combine_kernel, heads, helpers),
        [fast((2 * heads, length), F32), slot_shape],
        [stats, parts],
        flops=pairs // 8,
    )
    spread = swap(spread, "ctx")

    own_out = call(
        functools.partial(own_gradients_kernel, heads),
        [pltpu.HBM((width, length), F32)] * 2 + piece_shapes((rows, width), BF16, pltpu.HBM),
        [own, key, value, totals],
        position,
        [pltpu.VMEM((length, width), F32)] + [pltpu.VMEM((length, TILE), BF16)] * 2,
        flops=2 * pairs,
    )
    key_own, value_own, *query_own = own_out
    spread, key_own, value_own = lax.optimization_barrier((spread, key_own, value_own))
    query_own = exchange(query_own, helpers)

    terms, *pieces = call(
        functools.partial(routed_gradients_kernel, heads, helpers),
        [pltpu.HBM((helpers, blocks, CAPACITY, width), BF16)] + piece_shapes((2 * width, share), BF16, pltpu.HBM),
        [routed, key, value, spread, key_own, value_own],
        position,
        [pltpu.VMEM((width, length), F32)] * 4
        + [pltpu.VMEM((2, helpers, WIDE_TILE // group, CAPACITY, width), BF16)]
        + [pltpu.VMEM((heads, length, WIDE_TILE), BF16)] * 2
        + [pltpu.SemaphoreType.DMA((4,))],
        flops=5 * pairs,
        fast=4,
        hand_in=(4, 5),
        hand_out=(0,),
    )
    returned = swap(terms.reshape(blocks * helpers, CAPACITY, width), everyone)
    returned = returned.reshape(helpers, blocks, CAPACITY, width)

    pieces = exchange(pieces, helpers)

    (query_grad,) = call(
        functools.partial(finish_kernel, helpers),
        [pltpu.HBM((rows, features), BF16)],
        [picker, returned, *query_own],
        position,
        [pltpu.VMEM((helpers, rows, width), BF16), pltpu.SemaphoreType.DMA((helpers,))],
        hand_out=(0,),
    )
    key_grad, value_grad = call(
        functools.partial(place_kernel, helpers),
        [shape((share, features), BF16)] * 2,
        pieces,
        position,
    )
    return query_grad[None], key_grad[None], value_grad[None]


def solution(mesh):
    split = P(None, ("ctx", "help"), None)
    shared = P(None, "ctx", None)

    return jax.shard_map(
        per_device,
        mesh=mesh,
        in_specs=(split, shared, shared, split, split),
        out_specs=(split, split, split),
        check_vma=False,
    )
```
